512 devices in a mesh: group: 2 (over y), seq: 32 (over z, core), tensor: 8 (over x).
Axes of the slice: x: 8, y: 2, z: 16, core: 2. Of those that a mesh axis runs over, the one named last changes fastest.
The devices are a block of a 8x8x16 slice.
Arguments:
- query: bfloat16 [128, 7168], P(('group', 'seq'), 'tensor'), parts along dimension 0, may hold values from -5 to 5
- key_cache: bfloat16 [256, 256, 7168], P(('group', 'seq'), None, 'tensor'), parts along dimension 0, may hold values from -5 to 5
- value_cache: bfloat16 [256, 256, 7168], P(('group', 'seq'), None, 'tensor'), parts along dimension 0, may hold values from -6 to 6
- alibi_slopes: float32 [56], P('tensor'), may hold values from 0 to 1, as said below
- block_seq: int32 [256], P(('group', 'seq')), parts along dimension 0, may hold values from 0 to 63, as said below
- block_pos: int32 [256], P(('group', 'seq')), parts along dimension 0, may hold values from 0 to 16, as said below
- lengths: int32 [128], P('group'), parts along dimension 0, may hold values from 1 to 4352, as said below
- out_weight: bfloat16 [7168, 14336], P('tensor', 'seq'), may hold values from -0.5 to 0.5
Outputs:
- mixed: bfloat16 [128, 14336], P(('group', 'tensor'), 'seq'), parts along dimension 0
The draws below stay inside these ranges and needn't reach their ends.
There are 2 independent parts, one for each index of `group`. The reference program is written for one: setup_inputs(seed, part) draws one part's arguments, and reference() takes and returns one part's arrays. A program takes and returns all parts, laid end to end along the dimension named above; an argument that names none is the same for every part. Nothing has to cross between parts.
Inputs may be any that keep to these rules, and one draw needn't show every extreme that they name: `block_seq`: every sequence owns at least one block and at most 17; the blocks of sequence s have block_pos 0 to n_s - 1, each once. block_pos of a block is below the number of blocks its sequence owns. `lengths`: A sequence that owns n blocks has a length above 256 * (n - 1) and at most 256 * n. `alibi_slopes`: positive slopes.
All inputs are finite; a program needn't handle non-finite values.
Results may differ from the reference program's by a relative error of at most 0.0054.
Values may be sent and summed in bfloat16 or wider, within the bound.
A program may use at most 64 MiB of HBM per device.

```python
import math
import jax
import jax.numpy as jnp
from jax import lax

D = 14336
HEADS = 56
HEAD_DIM = 128
BLOCK = 256
SEQS = 64
BLOCKS = 128
MOST_BLOCKS = 17


def block_layout(key):
    second = jax.random.fold_in(key, 12)
    third = jax.random.fold_in(key, 13)
    fourth = jax.random.fold_in(key, 14)
    fifth = jax.random.fold_in(key, 15)
    extra = BLOCKS - SEQS
    capacity = MOST_BLOCKS - 1
    remain = extra - capacity
    relabel = jax.random.permutation(third, SEQS).astype(jnp.int32)
    longest = relabel[0]
    seq_ids = jnp.arange(SEQS, dtype=jnp.int32)
    counts = 1 + capacity * (seq_ids == longest).astype(jnp.int32)
    if remain > 0:
        order = jax.random.permutation(second, (SEQS - 1) * capacity)[:remain].astype(jnp.int32)
        target = relabel[1 + order // capacity]
        counts = counts + jnp.sum((target[:, None] == seq_ids[None, :]).astype(jnp.int32), axis=0)
    ends = jnp.cumsum(counts).astype(jnp.int32)
    starts = ends - counts
    slots = jnp.arange(BLOCKS, dtype=jnp.int32)
    seq_of = jnp.sum((ends[None, :] <= slots[:, None]).astype(jnp.int32), axis=1)
    pos_of = slots - starts[seq_of]
    placed = jax.random.permutation(fourth, BLOCKS)
    owners = jnp.zeros((BLOCKS,), jnp.int32).at[placed].set(seq_of)
    places = jnp.zeros((BLOCKS,), jnp.int32).at[placed].set(pos_of)
    tails = jax.random.randint(fifth, (SEQS,), 1, BLOCK + 1).astype(jnp.int32)
    tails = jnp.where(seq_ids == longest, BLOCK, tails)
    sizes_out = ((counts - 1) * BLOCK + tails).astype(jnp.int32)
    return (owners, places, sizes_out)


def draw_block_seq(key, part):
    return block_layout(key)[0]


def draw_block_pos(key, part):
    return block_layout(key)[1]


def draw_lengths(key, part):
    return block_layout(key)[2]


def draw_query(key, part):
    base = jnp.clip(jax.random.normal(jax.random.fold_in(key, 21), (SEQS, HEADS, HEAD_DIM), jnp.float32), -5.0, 5.0)
    return base.reshape(SEQS, HEADS * HEAD_DIM).astype(jnp.bfloat16)


def draw_key_cache(key, part):
    base = jnp.clip(jax.random.normal(jax.random.fold_in(key, 23), (BLOCKS, BLOCK, HEADS * HEAD_DIM), jnp.float32), -5.0, 5.0)
    return base.astype(jnp.bfloat16)


def draw_alibi_slopes(key, part):
    spread = jax.random.uniform(jax.random.fold_in(key, 32), (HEADS,), jnp.float32)
    strong = jax.random.randint(jax.random.fold_in(key, 31), (HEADS,), 0, 2) == 1
    slow = jnp.exp(jnp.log(1.0 / 8192.0) + spread * jnp.log(8.0))
    fast = jnp.exp(jnp.log(1.0 / 64.0) + spread * jnp.log(8.0))
    return jnp.where(strong, fast, slow).astype(jnp.float32)


def steps_of(rng, shape, shards, least, high):
    factor_of, own = 1.0, jax.random.fold_in(rng, 6)
    for axis_at, parts in shards:
        steps = jnp.exp(jax.random.uniform(jax.random.fold_in(own, axis_at), (parts,), jnp.float32, least / len(shards), high / len(shards)))
        factor_of = factor_of * jnp.repeat(steps, shape[axis_at] // parts).reshape([-1 if axis == axis_at else 1 for axis in range(len(shape))])
    return factor_of


def scatter_about(rng, extent, deviation, bound, split=(), kind=jnp.bfloat16):
    array = jax.random.normal(rng, extent, jnp.float32) * deviation
    if len(split) > 0:
        array = steps_of(rng, extent, split, -0.22, 0.18) * array
    return jnp.clip(array, min=-bound, max=bound).astype(kind)


def setup_inputs(seed: int = 0, part: int = 0) -> dict:
    streams_of = jax.random.split(jax.random.key(seed), 9)
    part_keys = jax.random.split(jax.random.fold_in(streams_of[8], part), 9)
    return {
        "query": draw_query(jax.random.fold_in(jax.random.fold_in(streams_of[8], part), 71), part),
        "key_cache": draw_key_cache(jax.random.fold_in(jax.random.fold_in(streams_of[8], part), 71), part),
        "value_cache": scatter_about(part_keys[2], (BLOCKS, BLOCK, HEADS * HEAD_DIM), 1.0, 6.0, ((0, 32), (2, 8))),
        "alibi_slopes": draw_alibi_slopes(jax.random.fold_in(streams_of[8], 71), part),
        "block_seq": draw_block_seq(jax.random.fold_in(jax.random.fold_in(streams_of[8], part), 71), part),
        "block_pos": draw_block_pos(jax.random.fold_in(jax.random.fold_in(streams_of[8], part), 71), part),
        "lengths": draw_lengths(jax.random.fold_in(jax.random.fold_in(streams_of[8], part), 71), part),
        "out_weight": scatter_about(streams_of[7], (HEADS * HEAD_DIM, D), HEAD_DIM ** -0.5, 0.5, ((0, 8), (1, 32))),
    }


def reference(query, key_cache, value_cache, alibi_slopes, block_seq, block_pos, lengths, out_weight):
    scale = 1.0 / math.sqrt(HEAD_DIM)
    offsets = jnp.arange(BLOCK, dtype=jnp.int32)

    def one_block(index):
        owner = block_seq[index]
        length = lengths[owner]
        placed = block_pos[index] * BLOCK + offsets
        live = placed < length
        qrow = query[owner].astype(jnp.float32).reshape(HEADS, HEAD_DIM)
        keys = key_cache[index].astype(jnp.float32).reshape(BLOCK, HEADS, HEAD_DIM)
        values = value_cache[index].astype(jnp.float32).reshape(BLOCK, HEADS, HEAD_DIM)
        scores = jnp.einsum('thd,hd->ht', keys, qrow) * scale
        distance = (length - 1 - placed).astype(jnp.float32)
        scores = scores - alibi_slopes[:, None] * distance[None, :]
        scores = jnp.where(live[None, :], scores, -1e+30)
        top = lax.optimization_barrier(jnp.max(scores, axis=1))
        weights = jnp.where(live[None, :], jnp.exp(scores - top[:, None]), 0.0)
        total = lax.optimization_barrier(jnp.sum(weights, axis=1))
        rounded = lax.optimization_barrier(weights.astype(jnp.bfloat16)).astype(jnp.float32)
        summed = jnp.einsum('ht,thd->hd', rounded, values)
        return (top, total, summed)
    tops, totals, sums = lax.map(one_block, jnp.arange(BLOCKS, dtype=jnp.int32))
    seq_ids = jnp.arange(SEQS, dtype=jnp.int32)
    owned = block_seq[None, :] == seq_ids[:, None]
    seq_max = lax.optimization_barrier(jnp.max(jnp.where(owned[:, :, None], tops[None], -1e+30), axis=1))
    factor = jnp.where(owned[:, :, None], jnp.exp(tops[None] - seq_max[:, None, :]), 0.0)
    seq_sum = lax.optimization_barrier(jnp.sum(factor * totals[None], axis=1))
    seq_acc = jnp.einsum('sbh,bhd->shd', factor, sums, precision=lax.Precision.HIGHEST)
    attention = (seq_acc / seq_sum[:, :, None]).reshape(SEQS, HEADS * HEAD_DIM).astype(jnp.bfloat16)
    return jnp.dot(attention, out_weight, preferred_element_type=jnp.float32).astype(jnp.bfloat16)
```

```python
import functools
import math

import jax
import jax.numpy as jnp
from jax import lax
from jax.experimental import pallas as pl
from jax.experimental.pallas import tpu as pltpu
from jax.sharding import PartitionSpec as P

MESH = pl.DeviceIdType.MESH
F32 = jnp.float32
BF16 = jnp.bfloat16
CORES = 2
GONE = -1e30


def remote(src, dst, send, recv, where):
    return pltpu.make_async_remote_copy(
        src_ref=src, dst_ref=dst, send_sem=send, recv_sem=recv, device_id=where, device_id_type=MESH
    )


def spread(slots, chips, z, c, send, recv, relay):
    def copy(k):
        there = lax.rem(z + k, chips) * CORES + c
        return remote(slots.at[c, z], slots.at[c, z], send.at[k], recv.at[k], {"seq": there})

    def start(i, _):
        far = chips // 2
        step = (i + 1) // 2
        k = jnp.where(lax.rem(i, 2) == 0, far - step, far + step)
        copy(k).start()
        return 0

    lax.fori_loop(0, chips - 1, start, 0)

    def arrive(k, _):
        copy(k).wait_recv()
        return 0

    lax.fori_loop(1, chips, arrive, 0)
    half = remote(slots.at[c], slots.at[c], relay.at[0], relay.at[1], {"seq": z * CORES + (1 - c)})
    half.start()
    half.wait_recv()

    def drain():
        def sent(k, _):
            copy(k).wait_send()
            return 0

        lax.fori_loop(1, chips, sent, 0)
        half.wait_send()

    return drain


def kernel(
    chips, owners, heads,
    q_hbm, k_hbm, v_hbm, slopes, block_seq, block_pos, lengths, w_hbm, out,
    kbuf, vbuf, wbuf, qall, gall, part, landed,
    load, q_send, q_recv, q_relay, g_send, g_recv, g_relay, p_send, p_recv,
):
    seq = lax.axis_index("seq")
    mine = lax.axis_index("tensor")
    z, c = seq // CORES, lax.rem(seq, CORES)
    blocks, block_len, features = k_hbm.shape
    rows = q_hbm.shape[0]
    head_dim = features // heads
    seqs = lengths.shape[0]
    scale = 1.0 / math.sqrt(head_dim)

    barrier = pltpu.get_barrier_semaphore()

    def greet_chip(k, _):
        there = lax.rem(z + k, chips) * CORES + c
        pl.semaphore_signal(barrier, inc=1, device_id={"seq": there}, device_id_type=MESH)
        return 0

    def greet_owner(k, _):
        there = lax.rem(mine + k, owners)
        pl.semaphore_signal(barrier, inc=1, device_id={"tensor": there}, device_id_type=MESH)
        return 0

    lax.fori_loop(1, chips, greet_chip, 0)
    pl.semaphore_signal(
        barrier, inc=1, device_id={"seq": z * CORES + (1 - c)}, device_id_type=MESH
    )
    lax.fori_loop(1, owners, greet_owner, 0)

    q_load = pltpu.make_async_copy(q_hbm, qall.at[c, z], load.at[0])
    k_load = pltpu.make_async_copy(k_hbm, kbuf, load.at[1])
    v_load = pltpu.make_async_copy(v_hbm, vbuf, load.at[2])
    w_load = pltpu.make_async_copy(w_hbm, wbuf, load.at[3])
    q_load.start()
    k_load.start()
    v_load.start()
    w_load.start()
    q_load.wait()
    pl.semaphore_wait(barrier, chips - 1 + 1 + owners - 1)

    q_drain = spread(qall, chips, z, c, q_send, q_recv, q_relay)

    sub = lax.broadcasted_iota(jnp.int32, (8, features), 0)
    lane = lax.broadcasted_iota(jnp.int32, (8, features), 1)
    own_head = lane // head_dim == sub
    t_at = lax.broadcasted_iota(jnp.int32, (8, block_len), 1)
    h_at = lax.broadcasted_iota(jnp.int32, (8, block_len), 0)
    slope = jnp.zeros((8, block_len), F32)
    for h in range(heads):
        slope = jnp.where(h_at == h, slopes[h], slope)
    a_sub = lax.broadcasted_iota(jnp.int32, (8, head_dim), 0)
    a_lane = lax.broadcasted_iota(jnp.int32, (8, head_dim), 1)

    k_load.wait()
    v_load.wait()
    wholes = []
    for b in range(blocks):
        s = block_seq[b]
        length = lengths[s]
        owner = s // rows
        r = lax.rem(s, rows)
        pair = qall[lax.rem(owner, CORES), owner // CORES].astype(F32)
        row = pair[0:1]
        for i in range(1, rows):
            row = jnp.where(r == i, pair[i : i + 1], row)
        wide = jnp.where(own_head, jnp.broadcast_to(row, (8, features)), 0.0).astype(BF16)
        scores = lax.dot_general(
            wide, kbuf[b], (((1,), (1,)), ((), ())), preferred_element_type=F32
        )
        placed = block_pos[b] * block_len + t_at
        live = placed < length
        distance = (length - 1 - placed).astype(F32)
        scores = jnp.where(live, scores * scale - slope * distance, GONE)
        top = jnp.max(scores, axis=1, keepdims=True)
        weights = jnp.where(live, jnp.exp(scores - top), 0.0)
        total = jnp.sum(weights, axis=1, keepdims=True)
        acc = jnp.dot(weights.astype(BF16), vbuf[b], preferred_element_type=F32)
        o = jnp.sum(jnp.where(own_head, acc / total, 0.0), axis=0, keepdims=True)
        lse = top + jnp.log(total)
        high = lse.astype(BF16).astype(F32)
        mid = (lse - high).astype(BF16).astype(F32)
        low = lse - high - mid
        tail = jnp.where(a_lane == a_sub, high, 0.0)
        tail = jnp.where(a_lane == a_sub + 8, mid, tail)
        tail = jnp.where(a_lane == a_sub + 16, low, tail)
        tail = jnp.where((a_lane == 24) & (a_sub == 0), s.astype(F32), tail)
        tail = jnp.sum(jnp.where(a_sub < heads, tail, 0.0), axis=0, keepdims=True)
        wholes.append(jnp.concatenate([o, tail], axis=1))

    wide = 2 * head_dim
    groups = (heads + 1) // 2
    m_sub = lax.broadcasted_iota(jnp.int32, (8, wide), 0)
    halves = []
    for first in range(0, groups * blocks, 8):
        half = jnp.zeros((8, wide), F32)
        for i in range(8):
            j, b = divmod(first + i, blocks)
            piece = wholes[b][:, j * wide : (j + 1) * wide]
            half = jnp.where(m_sub == i, jnp.broadcast_to(piece, (8, wide)), half)
        halves.append(half)
    gall[c, z] = jnp.concatenate(halves, axis=0).astype(BF16)

    g_drain = spread(gall, chips, z, c, g_send, g_recv, g_relay)

    high_rows = groups * blocks
    count = CORES * chips * high_rows
    both = gall[...].reshape(count, wide)
    p_sub = lax.broadcasted_iota(jnp.int32, (16, head_dim), 0)
    p_lane = lax.broadcasted_iota(jnp.int32, (16, head_dim), 1)
    pick = (p_sub < 8) & (p_lane < 24) & (lax.rem(p_lane, 8) == p_sub)
    pick = pick | ((p_sub == 8) & (p_lane == 24))
    pick = jnp.where(pick, 1.0, 0.0).astype(BF16)
    tails = lax.dot_general(
        pick, both[:, head_dim:], (((1,), (1,)), ((), ())), preferred_element_type=F32
    )
    column = lax.broadcasted_iota(jnp.int32, (seqs, count), 1)
    group_of = lax.rem(column // blocks, groups)
    seq_at = lax.broadcasted_iota(jnp.int32, (seqs, count), 0).astype(F32)
    shares = []
    for j in range(groups):
        back = (groups - 1 - j) * blocks
        moved = tails if back == 0 else pltpu.roll(tails, count - back, 1)
        mask = (group_of == j) & (jnp.broadcast_to(moved[8:9], (seqs, count)) == seq_at)
        for h in range(2 * j, min(2 * j + 2, heads)):
            level = jnp.where(mask, jnp.broadcast_to(moved[h : h + 1], (seqs, count)), GONE)
            best = jnp.max(level, axis=1, keepdims=True)
            share = jnp.exp(level - best)
            share = share / jnp.sum(share, axis=1, keepdims=True)
            shares.append(share.astype(BF16))
    mixed = jnp.dot(jnp.concatenate(shares, axis=0), both, preferred_element_type=F32)
    attention = jnp.concatenate(
        [
            mixed[h * seqs : (h + 1) * seqs, (h % 2) * head_dim : (h % 2 + 1) * head_dim].astype(BF16)
            for h in range(heads)
        ],
        axis=1,
    )
    w_load.wait()
    product = jnp.dot(attention, wbuf[...], preferred_element_type=F32)
    share_rows = seqs // owners
    for x in range(owners):
        part[x] = product[x * share_rows : (x + 1) * share_rows].astype(BF16)

    def give(k):
        there = lax.rem(mine + k, owners)
        return remote(part.at[there], landed.at[k], p_send.at[k], p_recv.at[k], {"tensor": there})

    def give_start(i, _):
        far = owners // 2
        step = (i + 1) // 2
        give(jnp.where(lax.rem(i, 2) == 0, far - step, far + step)).start()
        return 0

    lax.fori_loop(0, owners - 1, give_start, 0)
    result = part[mine].astype(F32)

    def give_arrive(k, _):
        give(k).wait_recv()
        return 0

    lax.fori_loop(1, owners, give_arrive, 0)
    for k in range(1, owners):
        result = result + landed[k].astype(F32)
    out[...] = result.astype(BF16)

    q_drain()
    g_drain()

    def give_sent(k, _):
        give(k).wait_send()
        return 0

    lax.fori_loop(1, owners, give_sent, 0)


def solution(mesh):
    chips = mesh.shape["seq"] // CORES
    owners = mesh.shape["tensor"]

    def local(query, key_cache, value_cache, alibi_slopes, block_seq, block_pos, lengths, out_weight):
        heads = alibi_slopes.shape[0]
        rows, features = query.shape
        blocks, block_len, _ = key_cache.shape
        seqs = lengths.shape[0]
        columns = out_weight.shape[1]
        head_dim = features // heads
        message = ((heads + 1) // 2 * blocks, 2 * head_dim)
        smem = pl.BlockSpec(memory_space=pltpu.SMEM)
        hbm = pl.BlockSpec(memory_space=pl.ANY)
        dma = pltpu.SemaphoreType.DMA
        return pl.pallas_call(
            functools.partial(kernel, chips, owners, heads),
            out_shape=jax.ShapeDtypeStruct((seqs // owners, columns), BF16),
            in_specs=[hbm, hbm, hbm, smem, smem, smem, smem, hbm],
            out_specs=pl.BlockSpec(memory_space=pltpu.VMEM),
            scratch_shapes=[
                pltpu.VMEM(key_cache.shape, BF16),
                pltpu.VMEM(value_cache.shape, BF16),
                pltpu.VMEM(out_weight.shape, BF16),
                pltpu.VMEM((CORES, chips, rows, features), BF16),
                pltpu.VMEM((CORES, chips, *message), BF16),
                pltpu.VMEM((owners, seqs // owners, columns), BF16),
                pltpu.VMEM((owners, seqs // owners, columns), BF16),
                dma((4,)),
                dma((chips,)),
                dma((chips,)),
                dma((2,)),
                dma((chips,)),
                dma((chips,)),
                dma((2,)),
                dma((owners,)),
                dma((owners,)),
            ],
            compiler_params=pltpu.CompilerParams(
                collective_id=0, has_side_effects=True, vmem_limit_bytes=32 * 1024 * 1024
            ),
        )(query, key_cache, value_cache, alibi_slopes, block_seq, block_pos, lengths, out_weight)

    placed = (
        P(("group", "seq"), "tensor"),
        P(("group", "seq"), None, "tensor"),
        P(("group", "seq"), None, "tensor"),
        P("tensor"),
        P(("group", "seq")),
        P(("group", "seq")),
        P("group"),
        P("tensor", "seq"),
    )
    return jax.shard_map(
        local, mesh=mesh, in_specs=placed, out_specs=P(("group", "tensor"), "seq"), check_vma=False
    )
```

```python
import functools
import math

import jax
import jax.numpy as jnp
from jax import lax
from jax.experimental import pallas as pl
from jax.experimental.pallas import tpu as pltpu
from jax.sharding import PartitionSpec as P

MESH = pl.DeviceIdType.MESH
F32 = jnp.float32
BF16 = jnp.bfloat16
CORES = 2
GONE = -1e30


def remote(src, dst, send, recv, where):
    return pltpu.make_async_remote_copy(
        src_ref=src, dst_ref=dst, send_sem=send, recv_sem=recv, device_id=where, device_id_type=MESH
    )


def spread(slots, chips, z, c, send, recv, relay):
    def copy(k):
        there = lax.rem(z + k, chips) * CORES + c
        return remote(slots.at[c, z], slots.at[c, z], send.at[k], recv.at[k], {"seq": there})

    def start(i, _):
        far = chips // 2
        step = (i + 1) // 2
        k = jnp.where(lax.rem(i, 2) == 0, far - step, far + step)
        copy(k).start()
        return 0

    lax.fori_loop(0, chips - 1, start, 0)

    def arrive(k, _):
        copy(k).wait_recv()
        return 0

    lax.fori_loop(1, chips, arrive, 0)
    half = remote(slots.at[c], slots.at[c], relay.at[0], relay.at[1], {"seq": z * CORES + (1 - c)})
    half.start()
    half.wait_recv()

    def drain():
        def sent(k, _):
            copy(k).wait_send()
            return 0

        lax.fori_loop(1, chips, sent, 0)
        half.wait_send()

    return drain


def kernel(
    chips, owners, heads,
    q_hbm, k_hbm, v_hbm, slopes_hbm, block_seq_hbm, block_pos_hbm, lengths_hbm, w_hbm, out,
    slopes, block_seq, block_pos, lengths, kbuf, vbuf, wbuf, qall, gall, part, landed,
    load, q_send, q_recv, q_relay, g_send, g_recv, g_relay, p_send, p_recv,
):
    seq = lax.axis_index("seq")
    mine = lax.axis_index("tensor")
    z, c = seq // CORES, lax.rem(seq, CORES)
    blocks, block_len, features = k_hbm.shape
    rows = q_hbm.shape[0]
    head_dim = features // heads
    seqs = lengths_hbm.shape[0]
    scale = 1.0 / math.sqrt(head_dim)

    barrier = pltpu.get_barrier_semaphore()

    def greet_chip(k, _):
        there = lax.rem(z + k, chips) * CORES + c
        pl.semaphore_signal(barrier, inc=1, device_id={"seq": there}, device_id_type=MESH)
        return 0

    def greet_owner(k, _):
        there = lax.rem(mine + k, owners)
        pl.semaphore_signal(barrier, inc=1, device_id={"tensor": there}, device_id_type=MESH)
        return 0

    lax.fori_loop(1, chips, greet_chip, 0)
    pl.semaphore_signal(
        barrier, inc=1, device_id={"seq": z * CORES + (1 - c)}, device_id_type=MESH
    )
    lax.fori_loop(1, owners, greet_owner, 0)

    q_load = pltpu.make_async_copy(q_hbm, qall.at[c, z], load.at[0])
    k_load = pltpu.make_async_copy(k_hbm, kbuf, load.at[1])
    v_load = pltpu.make_async_copy(v_hbm, vbuf, load.at[2])
    w_load = pltpu.make_async_copy(w_hbm, wbuf, load.at[3])
    small = [
        pltpu.make_async_copy(src, dst, load.at[4 + i])
        for i, (src, dst) in enumerate(
            (
                (slopes_hbm, slopes),
                (block_seq_hbm, block_seq),
                (block_pos_hbm, block_pos),
                (lengths_hbm, lengths),
            )
        )
    ]
    q_load.start()
    for copy in small:
        copy.start()
    k_load.start()
    v_load.start()
    w_load.start()
    q_load.wait()
    pl.semaphore_wait(barrier, chips - 1 + 1 + owners - 1)

    q_drain = spread(qall, chips, z, c, q_send, q_recv, q_relay)

    sub = lax.broadcasted_iota(jnp.int32, (8, features), 0)
    lane = lax.broadcasted_iota(jnp.int32, (8, features), 1)
    own_head = lane // head_dim == sub
    t_at = lax.broadcasted_iota(jnp.int32, (8, block_len), 1)
    h_at = lax.broadcasted_iota(jnp.int32, (8, block_len), 0)
    a_sub = lax.broadcasted_iota(jnp.int32, (8, head_dim), 0)
    a_lane = lax.broadcasted_iota(jnp.int32, (8, head_dim), 1)

    k_load.wait()
    v_load.wait()
    for copy in small:
        copy.wait()
    slope = jnp.zeros((8, block_len), F32)
    for h in range(heads):
        slope = jnp.where(h_at == h, slopes[h], slope)
    wholes = []
    for b in range(blocks):
        s = block_seq[b]
        length = lengths[s]
        owner = s // rows
        r = lax.rem(s, rows)
        pair = qall[lax.rem(owner, CORES), owner // CORES].astype(F32)
        row = pair[0:1]
        for i in range(1, rows):
            row = jnp.where(r == i, pair[i : i + 1], row)
        wide = jnp.where(own_head, jnp.broadcast_to(row, (8, features)), 0.0).astype(BF16)
        scores = lax.dot_general(
            wide, kbuf[b], (((1,), (1,)), ((), ())), preferred_element_type=F32
        )
        placed = block_pos[b] * block_len + t_at
        live = placed < length
        distance = (length - 1 - placed).astype(F32)
        scores = jnp.where(live, scores * scale - slope * distance, GONE)
        top = jnp.max(scores, axis=1, keepdims=True)
        weights = jnp.where(live, jnp.exp(scores - top), 0.0)
        total = jnp.sum(weights, axis=1, keepdims=True)
        acc = jnp.dot(weights.astype(BF16), vbuf[b], preferred_element_type=F32)
        o = jnp.sum(jnp.where(own_head, acc / total, 0.0), axis=0, keepdims=True)
        lse = top + jnp.log(total)
        high = lse.astype(BF16).astype(F32)
        mid = (lse - high).astype(BF16).astype(F32)
        low = lse - high - mid
        tail = jnp.where(a_lane == a_sub, high, 0.0)
        tail = jnp.where(a_lane == a_sub + 8, mid, tail)
        tail = jnp.where(a_lane == a_sub + 16, low, tail)
        tail = jnp.where((a_lane == 24) & (a_sub == 0), s.astype(F32), tail)
        tail = jnp.sum(jnp.where(a_sub < heads, tail, 0.0), axis=0, keepdims=True)
        wholes.append(jnp.concatenate([o, tail], axis=1))

    wide = 2 * head_dim
    groups = (heads + 1) // 2
    m_sub = lax.broadcasted_iota(jnp.int32, (8, wide), 0)
    halves = []
    for first in range(0, groups * blocks, 8):
        half = jnp.zeros((8, wide), F32)
        for i in range(8):
            j, b = divmod(first + i, blocks)
            piece = wholes[b][:, j * wide : (j + 1) * wide]
            half = jnp.where(m_sub == i, jnp.broadcast_to(piece, (8, wide)), half)
        halves.append(half)
    gall[c, z] = jnp.concatenate(halves, axis=0).astype(BF16)

    g_drain = spread(gall, chips, z, c, g_send, g_recv, g_relay)

    high_rows = groups * blocks
    count = CORES * chips * high_rows
    both = gall[...].reshape(count, wide)
    p_sub = lax.broadcasted_iota(jnp.int32, (16, head_dim), 0)
    p_lane = lax.broadcasted_iota(jnp.int32, (16, head_dim), 1)
    pick = (p_sub < 8) & (p_lane < 24) & (lax.rem(p_lane, 8) == p_sub)
    pick = pick | ((p_sub == 8) & (p_lane == 24))
    pick = jnp.where(pick, 1.0, 0.0).astype(BF16)
    tails = lax.dot_general(
        pick, both[:, head_dim:], (((1,), (1,)), ((), ())), preferred_element_type=F32
    )
    column = lax.broadcasted_iota(jnp.int32, (seqs, count), 1)
    group_of = lax.rem(column // blocks, groups)
    seq_at = lax.broadcasted_iota(jnp.int32, (seqs, count), 0).astype(F32)
    shares = []
    for j in range(groups):
        back = (groups - 1 - j) * blocks
        moved = tails if back == 0 else pltpu.roll(tails, count - back, 1)
        mask = (group_of == j) & (jnp.broadcast_to(moved[8:9], (seqs, count)) == seq_at)
        for h in range(2 * j, min(2 * j + 2, heads)):
            level = jnp.where(mask, jnp.broadcast_to(moved[h : h + 1], (seqs, count)), GONE)
            best = jnp.max(level, axis=1, keepdims=True)
            share = jnp.exp(level - best)
            share = share / jnp.sum(share, axis=1, keepdims=True)
            shares.append(share.astype(BF16))
    mixed = jnp.dot(jnp.concatenate(shares, axis=0), both, preferred_element_type=F32)
    attention = jnp.concatenate(
        [
            mixed[h * seqs : (h + 1) * seqs, (h % 2) * head_dim : (h % 2 + 1) * head_dim].astype(BF16)
            for h in range(heads)
        ],
        axis=1,
    )
    w_load.wait()
    product = lax.dot_general(
        attention, wbuf[...], (((1,), (1,)), ((), ())), preferred_element_type=F32
    )
    share_rows = seqs // owners
    for x in range(owners):
        part[x] = product[x * share_rows : (x + 1) * share_rows].astype(BF16)

    def give(k):
        there = lax.rem(mine + k, owners)
        return remote(part.at[there], landed.at[k], p_send.at[k], p_recv.at[k], {"tensor": there})

    def give_start(i, _):
        far = owners // 2
        step = (i + 1) // 2
        give(jnp.where(lax.rem(i, 2) == 0, far - step, far + step)).start()
        return 0

    lax.fori_loop(0, owners - 1, give_start, 0)
    result = part[mine].astype(F32)

    def give_arrive(k, _):
        give(k).wait_recv()
        return 0

    lax.fori_loop(1, owners, give_arrive, 0)
    for k in range(1, owners):
        result = result + landed[k].astype(F32)
    out[...] = result.astype(BF16)

    q_drain()
    g_drain()

    def give_sent(k, _):
        give(k).wait_send()
        return 0

    lax.fori_loop(1, owners, give_sent, 0)


def solution(mesh):
    chips = mesh.shape["seq"] // CORES
    owners = mesh.shape["tensor"]

    def local(query, key_cache, value_cache, alibi_slopes, block_seq, block_pos, lengths, out_weight):
        heads = alibi_slopes.shape[0]
        rows, features = query.shape
        blocks, block_len, _ = key_cache.shape
        seqs = lengths.shape[0]
        columns = out_weight.shape[1]
        head_dim = features // heads
        message = ((heads + 1) // 2 * blocks, 2 * head_dim)
        hbm = pl.BlockSpec(memory_space=pltpu.HBM)
        dma = pltpu.SemaphoreType.DMA
        return pl.pallas_call(
            functools.partial(kernel, chips, owners, heads),
            out_shape=jax.ShapeDtypeStruct((seqs // owners, columns), BF16),
            in_specs=[hbm] * 8,
            out_specs=pl.BlockSpec(memory_space=pltpu.VMEM),
            scratch_shapes=[
                pltpu.SMEM(alibi_slopes.shape, F32),
                pltpu.SMEM(block_seq.shape, jnp.int32),
                pltpu.SMEM(block_pos.shape, jnp.int32),
                pltpu.SMEM(lengths.shape, jnp.int32),
                pltpu.VMEM(key_cache.shape, BF16),
                pltpu.VMEM(value_cache.shape, BF16),
                pltpu.VMEM(out_weight.shape[::-1], BF16),
                pltpu.VMEM((CORES, chips, rows, features), BF16),
                pltpu.VMEM((CORES, chips, *message), BF16),
                pltpu.VMEM((owners, seqs // owners, columns), BF16),
                pltpu.VMEM((owners, seqs // owners, columns), BF16),
                dma((8,)),
                dma((chips,)),
                dma((chips,)),
                dma((2,)),
                dma((chips,)),
                dma((chips,)),
                dma((2,)),
                dma((owners,)),
                dma((owners,)),
            ],
            compiler_params=pltpu.CompilerParams(
                collective_id=0, has_side_effects=True
            ),
        )(query, key_cache, value_cache, alibi_slopes, block_seq, block_pos, lengths, out_weight.T)

    placed = (
        P(("group", "seq"), "tensor"),
        P(("group", "seq"), None, "tensor"),
        P(("group", "seq"), None, "tensor"),
        P("tensor"),
        P(("group", "seq")),
        P(("group", "seq")),
        P("group"),
        P("tensor", "seq"),
    )
    return jax.shard_map(
        local, mesh=mesh, in_specs=placed, out_specs=P(("group", "tensor"), "seq"), check_vma=False
    )
```

```python
import functools
import math

import jax
import jax.numpy as jnp
from jax import lax
from jax.experimental import pallas as pl
from jax.experimental.pallas import tpu as pltpu
from jax.sharding import PartitionSpec as P

MESH = pl.DeviceIdType.MESH
F32 = jnp.float32
BF16 = jnp.bfloat16
CORES = 2
GONE = -1e30


def remote(src, dst, send, recv, where):
    return pltpu.make_async_remote_copy(
        src_ref=src, dst_ref=dst, send_sem=send, recv_sem=recv, device_id=where, device_id_type=MESH
    )


def spread(slots, chips, z, c, send, recv, relay):
    def copy(k):
        there = lax.rem(z + k, chips) * CORES + c
        return remote(slots.at[c, z], slots.at[c, z], send, recv.at[k], {"seq": there})

    for k in far_first(chips):
        copy(k).start()
    for k in range(1, chips):
        copy(k).wait_recv()
    partner = {"seq": z * CORES + 1 - c}
    half = remote(slots.at[c], slots.at[c], relay.at[0], relay.at[1], partner)
    half.start()
    half.wait_recv()

    def drain():
        every = pl.ds(0, chips - 1)
        remote(slots.at[c, every], slots.at[c, every], send, relay.at[1], partner).wait_send()
        half.wait_send()

    return drain


def far_first(n):
    return sorted(range(1, n), key=lambda m: -min(m, n - m))


def kernel(
    chips, owners, heads,
    q_hbm, k_hbm, v_hbm, slopes_hbm, block_seq_hbm, block_pos_hbm, lengths_hbm, w_hbm, out,
    slopes, block_seq, block_pos, lengths, kbuf, vbuf, wbuf, qall, gall, part, landed,
    load, met, e_send, e_recv, q_send, q_recv, g_send, g_recv, g_relay, p_send, p_recv,
):
    seq = lax.axis_index("seq")
    mine = lax.axis_index("tensor")
    devices = CORES * chips
    z, c = seq // CORES, lax.rem(seq, CORES)
    blocks, block_len, features = k_hbm.shape
    rows = q_hbm.shape[0]
    head_dim = features // heads
    seqs = lengths_hbm.shape[0]
    scale = 1.0 / math.sqrt(head_dim)

    near = jnp.minimum(mine, owners - mine)
    rank = jnp.where(mine * 2 > owners, 2 * near - 1, jnp.where(mine * 2 == owners, owners - 1, 2 * near))

    def owner_of(r):
        half = (r + 1) // 2
        return jnp.where(r == owners - 1, owners // 2, jnp.where(lax.rem(r, 2) == 1, owners - half, half))

    place = lax.rem(seq + devices - 1, devices)
    last = chips - 1

    barrier = pltpu.get_barrier_semaphore()

    def greet_seq(at, _):
        there = lax.rem(at + 1, devices)
        pl.semaphore_signal(barrier, inc=1, device_id={"seq": there}, device_id_type=MESH)
        return 0

    def greet_owner(r, _):
        pl.semaphore_signal(
            barrier, inc=1, device_id={"tensor": owner_of(r)}, device_id_type=MESH
        )
        return 0

    q_load = pltpu.make_async_copy(q_hbm, qall.at[seq], load.at[0])
    q_load.start()
    lax.fori_loop(place + 1, devices, greet_seq, 0)
    lax.fori_loop(rank + 1, owners, greet_owner, 0)

    small = [
        pltpu.make_async_copy(src, dst, load.at[4 + i])
        for i, (src, dst) in enumerate(
            (
                (slopes_hbm, slopes),
                (block_seq_hbm, block_seq),
                (block_pos_hbm, block_pos),
                (lengths_hbm, lengths),
            )
        )
    ]
    k_load = pltpu.make_async_copy(k_hbm, kbuf, load.at[1])
    v_load = pltpu.make_async_copy(v_hbm, vbuf, load.at[2])
    w_load = pltpu.make_async_copy(w_hbm, wbuf, load.at[3])
    for copy in small:
        copy.start()
    k_load.start()
    v_load.start()
    w_load.start()
    q_load.wait()

    @pl.when(place + rank > 0)
    def _():
        pl.semaphore_wait(barrier, place + rank)

    def give_q(j):
        return remote(qall.at[seq], qall.at[seq], q_send, q_recv.at[seq], {"seq": j})

    def arrival(j):
        return remote(qall.at[j], qall.at[j], q_send, q_recv.at[j], {"seq": z * CORES + 1 - c})

    def send_down(i, _):
        far = chips // 2
        step = (i + 1) // 2
        k = jnp.where(lax.rem(i, 2) == 0, far - step, far + step)
        for cc in range(CORES):
            j = lax.rem(z + k, chips) * CORES + cc

            @pl.when(lax.rem(j + devices - 1, devices) < place)
            def _():
                give_q(j).start()

        return 0

    lax.fori_loop(0, chips, send_down, 0)

    def hail_owner(r, _):
        pl.semaphore_signal(met, inc=1, device_id={"tensor": owner_of(r)}, device_id_type=MESH)
        return 0

    lax.fori_loop(0, rank, hail_owner, 0)

    early = pl.ds(1, (last - 1) * CORES - 1)

    def bulk(j, i):
        return remote(qall.at[early], qall.at[early], e_send.at[i], e_recv, {"seq": j})

    def send_up(at, _):
        j = lax.rem(at + 1, devices)
        arrival(j).wait_recv()

        @pl.when((j // CORES != last) | (z >= last - 1) | (seq == 0))
        def _():
            give_q(j).start()

        return 0

    lax.fori_loop(place + 1, devices - CORES - 1, send_up, 0)
    lax.fori_loop(jnp.maximum(place + 1, devices - CORES - 1), devices - 1, send_up, 0)

    @pl.when(seq == 1)
    def _():
        for i in range(CORES):
            bulk(last * CORES + i, i).start()

    @pl.when(place < devices - 1)
    def _():
        send_up(devices - 1, 0)

    def arrive(at, _):
        arrival(lax.rem(at + 1, devices)).wait_recv()
        return 0

    @pl.when(z == last)
    def _():
        bulk(seq, 0).wait_recv()
        lax.fori_loop((last - 1) * CORES - 1, place, arrive, 0)

    @pl.when(z != last)
    def _():
        lax.fori_loop(0, place, arrive, 0)

    def q_drain():
        @pl.when((z >= last - 1) | (seq == 0))
        def _():
            every = pl.ds(0, devices - 1)
            remote(qall.at[every], qall.at[every], q_send, e_recv, {"seq": z * CORES + 1 - c}).wait_send()

        @pl.when((z < last - 1) & (seq != 0))
        def _():
            every = pl.ds(0, devices - 1 - CORES)
            remote(qall.at[every], qall.at[every], q_send, e_recv, {"seq": z * CORES + 1 - c}).wait_send()

        @pl.when(seq == 1)
        def _():
            for i in range(CORES):
                bulk(last * CORES + i, i).wait_send()

    sub = lax.broadcasted_iota(jnp.int32, (8, features), 0)
    lane = lax.broadcasted_iota(jnp.int32, (8, features), 1)
    own_head = lane // head_dim == sub
    t_at = lax.broadcasted_iota(jnp.int32, (8, block_len), 1)
    h_at = lax.broadcasted_iota(jnp.int32, (8, block_len), 0)
    a_sub = lax.broadcasted_iota(jnp.int32, (8, head_dim), 0)
    a_lane = lax.broadcasted_iota(jnp.int32, (8, head_dim), 1)

    k_load.wait()
    v_load.wait()
    for copy in small:
        copy.wait()
    slope = jnp.zeros((8, block_len), F32)
    for h in range(heads):
        slope = jnp.where(h_at == h, slopes[h], slope)
    wholes = []
    for b in range(blocks):
        s = block_seq[b]
        length = lengths[s]
        owner = s // rows
        r = lax.rem(s, rows)
        pair = qall[owner].astype(F32)
        row = pair[0:1]
        for i in range(1, rows):
            row = jnp.where(r == i, pair[i : i + 1], row)
        wide = jnp.where(own_head, jnp.broadcast_to(row, (8, features)), 0.0).astype(BF16)
        scores = lax.dot_general(
            wide, kbuf[b], (((1,), (1,)), ((), ())), preferred_element_type=F32
        )
        placed = block_pos[b] * block_len + t_at
        live = placed < length
        distance = (length - 1 - placed).astype(F32)
        scores = jnp.where(live, scores * scale - slope * distance, GONE)
        top = jnp.max(scores, axis=1, keepdims=True)
        weights = jnp.where(live, jnp.exp(scores - top), 0.0)
        total = jnp.sum(weights, axis=1, keepdims=True)
        acc = jnp.dot(weights.astype(BF16), vbuf[b], preferred_element_type=F32)
        o = jnp.sum(jnp.where(own_head, acc / total, 0.0), axis=0, keepdims=True)
        lse = top + jnp.log(total)
        high = lse.astype(BF16).astype(F32)
        mid = (lse - high).astype(BF16).astype(F32)
        low = lse - high - mid
        tail = jnp.where(a_lane == a_sub, high, 0.0)
        tail = jnp.where(a_lane == a_sub + 8, mid, tail)
        tail = jnp.where(a_lane == a_sub + 16, low, tail)
        tail = jnp.where((a_lane == 24) & (a_sub == 0), s.astype(F32), tail)
        tail = jnp.sum(jnp.where(a_sub < heads, tail, 0.0), axis=0, keepdims=True)
        wholes.append(jnp.concatenate([o, tail], axis=1))

    wide = 2 * head_dim
    groups = (heads + 1) // 2
    m_sub = lax.broadcasted_iota(jnp.int32, (8, wide), 0)
    halves = []
    for first in range(0, groups * blocks, 8):
        half = jnp.zeros((8, wide), F32)
        for i in range(8):
            j, b = divmod(first + i, blocks)
            piece = wholes[b][:, j * wide : (j + 1) * wide]
            half = jnp.where(m_sub == i, jnp.broadcast_to(piece, (8, wide)), half)
        halves.append(half)
    gall[c, z] = jnp.concatenate(halves, axis=0).astype(BF16)

    g_drain = spread(gall, chips, z, c, g_send, g_recv, g_relay)

    high_rows = groups * blocks
    count = CORES * chips * high_rows
    both = gall[...].reshape(count, wide)
    p_sub = lax.broadcasted_iota(jnp.int32, (16, head_dim), 0)
    p_lane = lax.broadcasted_iota(jnp.int32, (16, head_dim), 1)
    pick = (p_sub < 8) & (p_lane < 24) & (lax.rem(p_lane, 8) == p_sub)
    pick = pick | ((p_sub == 8) & (p_lane == 24))
    pick = jnp.where(pick, 1.0, 0.0).astype(BF16)
    tails = lax.dot_general(
        pick, both[:, head_dim:], (((1,), (1,)), ((), ())), preferred_element_type=F32
    )
    column = lax.broadcasted_iota(jnp.int32, (seqs, count), 1)
    group_of = lax.rem(column // blocks, groups)
    seq_at = lax.broadcasted_iota(jnp.int32, (seqs, count), 0).astype(F32)
    shares = []
    for j in range(groups):
        back = (groups - 1 - j) * blocks
        moved = tails if back == 0 else pltpu.roll(tails, count - back, 1)
        mask = (group_of == j) & (jnp.broadcast_to(moved[8:9], (seqs, count)) == seq_at)
        for h in range(2 * j, min(2 * j + 2, heads)):
            level = jnp.where(mask, jnp.broadcast_to(moved[h : h + 1], (seqs, count)), GONE)
            best = jnp.max(level, axis=1, keepdims=True)
            share = jnp.exp(level - best)
            share = share / jnp.sum(share, axis=1, keepdims=True)
            shares.append(share.astype(BF16))
    mixed = jnp.dot(jnp.concatenate(shares, axis=0), both, preferred_element_type=F32)
    attention = jnp.concatenate(
        [
            mixed[h * seqs : (h + 1) * seqs, (h % 2) * head_dim : (h % 2 + 1) * head_dim].astype(BF16)
            for h in range(heads)
        ],
        axis=1,
    )
    w_load.wait()
    product = lax.dot_general(
        attention, wbuf[...], (((1,), (1,)), ((), ())), preferred_element_type=F32
    )
    share_rows = seqs // owners
    for x in range(owners):
        part[x] = product[x * share_rows : (x + 1) * share_rows].astype(BF16)

    def give(k):
        there = lax.rem(mine + k, owners)
        return remote(part.at[there], landed.at[k], p_send.at[k], p_recv.at[k], {"tensor": there})

    @pl.when(rank < owners - 1)
    def _():
        pl.semaphore_wait(met, owners - 1 - rank)

    for k in far_first(owners):
        give(k).start()
    result = part[mine].astype(F32)

    for k in range(1, owners):
        give(k).wait_recv()
        result = result + landed[k].astype(F32)
    out[...] = result.astype(BF16)

    q_drain()
    g_drain()

    for k in range(1, owners):
        give(k).wait_send()


def solution(mesh):
    chips = mesh.shape["seq"] // CORES
    owners = mesh.shape["tensor"]

    def local(query, key_cache, value_cache, alibi_slopes, block_seq, block_pos, lengths, out_weight):
        heads = alibi_slopes.shape[0]
        rows, features = query.shape
        blocks, block_len, _ = key_cache.shape
        seqs = lengths.shape[0]
        columns = out_weight.shape[1]
        head_dim = features // heads
        message = ((heads + 1) // 2 * blocks, 2 * head_dim)
        hbm = pl.BlockSpec(memory_space=pltpu.HBM)
        dma = pltpu.SemaphoreType.DMA
        return pl.pallas_call(
            functools.partial(kernel, chips, owners, heads),
            out_shape=pltpu.VMEM((seqs // owners, columns), BF16),
            in_specs=[hbm] * 8,
            out_specs=pl.BlockSpec(memory_space=pltpu.VMEM),
            scratch_shapes=[
                pltpu.SMEM(alibi_slopes.shape, F32),
                pltpu.SMEM(block_seq.shape, jnp.int32),
                pltpu.SMEM(block_pos.shape, jnp.int32),
                pltpu.SMEM(lengths.shape, jnp.int32),
                pltpu.VMEM(key_cache.shape, BF16),
                pltpu.VMEM(value_cache.shape, BF16),
                pltpu.VMEM(out_weight.shape[::-1], BF16),
                pltpu.VMEM((CORES * chips, rows, features), BF16),
                pltpu.VMEM((CORES, chips, *message), BF16),
                pltpu.VMEM((owners, seqs // owners, columns), BF16),
                pltpu.VMEM((owners, seqs // owners, columns), BF16),
                dma((8,)),
                pltpu.SemaphoreType.REGULAR,
                dma((CORES,)),
                dma,
                dma,
                dma((CORES * chips,)),
                dma,
                dma((chips,)),
                dma((2,)),
                dma((owners,)),
                dma((owners,)),
            ],
            compiler_params=pltpu.CompilerParams(
                collective_id=0, has_side_effects=True
            ),
        )(query, key_cache, value_cache, alibi_slopes, block_seq, block_pos, lengths, out_weight.T)

    placed = (
        P(("group", "seq"), "tensor"),
        P(("group", "seq"), None, "tensor"),
        P(("group", "seq"), None, "tensor"),
        P("tensor"),
        P(("group", "seq")),
        P(("group", "seq")),
        P("group"),
        P("tensor", "seq"),
    )
    return jax.shard_map(
        local, mesh=mesh, in_specs=placed, out_specs=P(("group", "tensor"), "seq"), check_vma=False
    )
```

```python
import functools
import math

import jax
import jax.numpy as jnp
from jax import lax
from jax.experimental import pallas as pl
from jax.experimental.pallas import tpu as pltpu
from jax.sharding import PartitionSpec as P

MESH = pl.DeviceIdType.MESH
F32 = jnp.float32
BF16 = jnp.bfloat16
CORES = 2
GONE = -1e30


def remote(src, dst, send, recv, where):
    return pltpu.make_async_remote_copy(
        src_ref=src, dst_ref=dst, send_sem=send, recv_sem=recv, device_id=where, device_id_type=MESH
    )


def spread(slots, chips, z, c, send, recv, relay):
    def copy(k):
        there = lax.rem(z + k, chips) * CORES + c
        return remote(slots.at[c, z], slots.at[c, z], send, recv.at[k], {"seq": there})

    for k in far_first(chips):
        copy(k).start()
    for k in range(1, chips):
        copy(k).wait_recv()
    partner = {"seq": z * CORES + 1 - c}
    half = remote(slots.at[c], slots.at[c], relay.at[0], relay.at[1], partner)
    half.start()
    half.wait_recv()

    def drain():
        every = pl.ds(0, chips - 1)
        remote(slots.at[c, every], slots.at[c, every], send, relay.at[1], partner).wait_send()
        half.wait_send()

    return drain


def far_first(n):
    return sorted(range(1, n), key=lambda m: -min(m, n - m))


def kernel(
    chips, owners, heads,
    q_hbm, k_hbm, v_hbm, slopes_hbm, block_seq_hbm, block_pos_hbm, lengths_hbm, w_hbm, out,
    slopes, block_seq, block_pos, lengths, kbuf, kturn, vbuf, wbuf, qall, gall, part, landed,
    load, met, f_send, f_recv, e_recv, r_recv, q_send, q_recv, g_send, g_recv, g_relay, p_send, p_recv,
):
    seq = lax.axis_index("seq")
    mine = lax.axis_index("tensor")
    devices = CORES * chips
    z, c = seq // CORES, lax.rem(seq, CORES)
    blocks, block_len, features = k_hbm.shape
    rows = q_hbm.shape[0]
    head_dim = features // heads
    seqs = lengths_hbm.shape[0]
    scale = 1.0 / math.sqrt(head_dim)

    near = jnp.minimum(mine, owners - mine)
    rank = jnp.where(mine * 2 > owners, 2 * near - 1, jnp.where(mine * 2 == owners, owners - 1, 2 * near))

    def owner_of(r):
        half = (r + 1) // 2
        return jnp.where(r == owners - 1, owners // 2, jnp.where(lax.rem(r, 2) == 1, owners - half, half))

    last = chips - 1

    barrier = pltpu.get_barrier_semaphore()

    def greet_seq(j, _):
        pl.semaphore_signal(barrier, inc=1, device_id={"seq": j}, device_id_type=MESH)
        return 0

    def greet_owner(r, _):
        pl.semaphore_signal(
            barrier, inc=1, device_id={"tensor": owner_of(r)}, device_id_type=MESH
        )
        return 0

    q_load = pltpu.make_async_copy(q_hbm, qall.at[seq], load.at[0])
    q_load.start()

    @pl.when(seq > 0)
    def _():
        lax.fori_loop(seq + 1, devices, greet_seq, 0)

    @pl.when(seq == 1)
    def _():
        greet_seq(0, 0)

    lax.fori_loop(rank + 1, owners, greet_owner, 0)

    small = [
        pltpu.make_async_copy(src, dst, load.at[4 + i])
        for i, (src, dst) in enumerate(
            (
                (slopes_hbm, slopes),
                (block_seq_hbm, block_seq),
                (block_pos_hbm, block_pos),
                (lengths_hbm, lengths),
            )
        )
    ]
    k_load = pltpu.make_async_copy(k_hbm, kbuf, load.at[1])
    v_load = pltpu.make_async_copy(v_hbm, vbuf, load.at[2])
    w_load = pltpu.make_async_copy(w_hbm, wbuf, load.at[3])
    for copy in small:
        copy.start()
    k_load.start()
    v_load.start()
    w_load.start()
    q_load.wait()
    before = jnp.where(seq == 0, 1, seq - 1) + rank

    @pl.when(before > 0)
    def _():
        pl.semaphore_wait(barrier, before)

    def give_q(j):
        return remote(qall.at[seq], qall.at[seq], q_send, q_recv.at[seq], {"seq": j})

    def arrival(j):
        return remote(qall.at[j], qall.at[j], q_send, q_recv.at[j], {"seq": z * CORES + 1 - c})

    def several(slots, recv, j, send=q_send):
        return remote(qall.at[slots], qall.at[slots], send, recv, {"seq": j})

    pair = pl.ds(0, CORES)
    rest = pl.ds(1, devices - 1)
    early = pl.ds(0, (last - 1) * CORES)

    def send_down(i, _):
        far = chips // 2
        step = (i + 1) // 2
        k = jnp.where(lax.rem(i, 2) == 0, far - step, far + step)
        for cc in range(CORES):
            j = lax.rem(z + k, chips) * CORES + cc

            @pl.when((j > 0) & (j < seq))
            def _():
                give_q(j).start()

        return 0

    lax.fori_loop(0, chips, send_down, 0)

    def hail_owner(r, _):
        pl.semaphore_signal(met, inc=1, device_id={"tensor": owner_of(r)}, device_id_type=MESH)
        return 0

    lax.fori_loop(0, rank, hail_owner, 0)

    k_load.wait()
    for b in range(blocks):
        kturn[b] = kbuf[b].T

    def arrive(j, _):
        arrival(j).wait_recv()
        return 0

    @pl.when(seq == 0)
    def _():
        give_q(1).start()
        several(rest, r_recv, 1).wait_recv()

    @pl.when(seq == 1)
    def _():
        arrival(0).wait_recv()

        def pass_pair(j, _):
            arrival(j).wait_recv()
            several(pair, f_recv, j, f_send).start()
            return 0

        lax.fori_loop(CORES, last * CORES, pass_pair, 0)

        def pass_early(j, _):
            arrival(j).wait_recv()
            several(early, e_recv, j, f_send).start()
            return 0

        lax.fori_loop(last * CORES, devices, pass_early, 0)
        several(rest, r_recv, 0).start()

    @pl.when(seq > 1)
    def _():
        def send_up(j, _):
            arrival(j).wait_recv()

            @pl.when((j // CORES != last) | (z >= last - 1))
            def _():
                give_q(j).start()

            return 0

        lax.fori_loop(seq + 1, devices, send_up, 0)

        @pl.when(z == last)
        def _():
            several(early, e_recv, 1).wait_recv()
            lax.fori_loop((last - 1) * CORES, seq, arrive, 0)

        @pl.when(z != last)
        def _():
            several(pair, f_recv, 1).wait_recv()
            lax.fori_loop(CORES, seq, arrive, 0)

    def q_drain():
        far = (last - 1) * CORES

        @pl.when(seq == 0)
        def _():
            give_q(1).wait_send()

        @pl.when(seq == 1)
        def _():
            several(rest, r_recv, 0).wait_send()
            size = kbuf.at[0, pl.ds(0, 2 * CORES * far * rows)]
            remote(size, size, f_send, r_recv, {"seq": 0}).wait_send()

        @pl.when((seq > 1) & (z < last - 1))
        def _():
            several(pl.ds(0, devices - 2 - CORES), r_recv, 1).wait_send()

        @pl.when(z >= last - 1)
        def _():
            several(pl.ds(0, devices - 2), r_recv, 1).wait_send()

    sub = lax.broadcasted_iota(jnp.int32, (8, features), 0)
    lane = lax.broadcasted_iota(jnp.int32, (8, features), 1)
    own_head = lane // head_dim == sub
    t_at = lax.broadcasted_iota(jnp.int32, (8, block_len), 1)
    h_at = lax.broadcasted_iota(jnp.int32, (8, block_len), 0)
    a_sub = lax.broadcasted_iota(jnp.int32, (8, head_dim), 0)
    a_lane = lax.broadcasted_iota(jnp.int32, (8, head_dim), 1)

    v_load.wait()
    for copy in small:
        copy.wait()
    slope = jnp.zeros((8, block_len), F32)
    for h in range(heads):
        slope = jnp.where(h_at == h, slopes[h], slope)
    wholes = []
    for b in range(blocks):
        s = block_seq[b]
        length = lengths[s]
        owner = s // rows
        r = lax.rem(s, rows)
        pair = qall[owner].astype(F32)
        row = pair[0:1]
        for i in range(1, rows):
            row = jnp.where(r == i, pair[i : i + 1], row)
        wide = jnp.where(own_head, jnp.broadcast_to(row, (8, features)), 0.0).astype(BF16)
        scores = lax.dot_general(
            wide, kturn[b], (((1,), (0,)), ((), ())), preferred_element_type=F32
        )
        placed = block_pos[b] * block_len + t_at
        live = placed < length
        distance = (length - 1 - placed).astype(F32)
        scores = jnp.where(live, scores * scale - slope * distance, GONE)
        top = jnp.max(scores, axis=1, keepdims=True)
        weights = jnp.where(live, jnp.exp(scores - top), 0.0)
        total = jnp.sum(weights, axis=1, keepdims=True)
        acc = jnp.dot(weights.astype(BF16), vbuf[b], preferred_element_type=F32)
        o = jnp.sum(jnp.where(own_head, acc / total, 0.0), axis=0, keepdims=True)
        lse = top + jnp.log(total)
        high = lse.astype(BF16).astype(F32)
        mid = (lse - high).astype(BF16).astype(F32)
        low = lse - high - mid
        tail = jnp.where(a_lane == a_sub, high, 0.0)
        tail = jnp.where(a_lane == a_sub + 8, mid, tail)
        tail = jnp.where(a_lane == a_sub + 16, low, tail)
        tail = jnp.where((a_lane == 24) & (a_sub == 0), s.astype(F32), tail)
        tail = jnp.sum(jnp.where(a_sub < heads, tail, 0.0), axis=0, keepdims=True)
        wholes.append(jnp.concatenate([o, tail], axis=1))

    wide = 2 * head_dim
    groups = (heads + 1) // 2
    m_sub = lax.broadcasted_iota(jnp.int32, (8, wide), 0)
    halves = []
    for first in range(0, groups * blocks, 8):
        half = jnp.zeros((8, wide), F32)
        for i in range(8):
            j, b = divmod(first + i, blocks)
            piece = wholes[b][:, j * wide : (j + 1) * wide]
            half = jnp.where(m_sub == i, jnp.broadcast_to(piece, (8, wide)), half)
        halves.append(half)
    gall[c, z] = jnp.concatenate(halves, axis=0).astype(BF16)

    g_drain = spread(gall, chips, z, c, g_send, g_recv, g_relay)

    high_rows = groups * blocks
    count = CORES * chips * high_rows
    both = gall[...].reshape(count, wide)
    p_sub = lax.broadcasted_iota(jnp.int32, (16, head_dim), 0)
    p_lane = lax.broadcasted_iota(jnp.int32, (16, head_dim), 1)
    pick = (p_sub < 8) & (p_lane < 24) & (lax.rem(p_lane, 8) == p_sub)
    pick = pick | ((p_sub == 8) & (p_lane == 24))
    pick = jnp.where(pick, 1.0, 0.0).astype(BF16)
    tails = lax.dot_general(
        pick, both[:, head_dim:], (((1,), (1,)), ((), ())), preferred_element_type=F32
    )
    column = lax.broadcasted_iota(jnp.int32, (seqs, count), 1)
    group_of = lax.rem(column // blocks, groups)
    seq_at = lax.broadcasted_iota(jnp.int32, (seqs, count), 0).astype(F32)
    shares = []
    for j in range(groups):
        back = (groups - 1 - j) * blocks
        moved = tails if back == 0 else pltpu.roll(tails, count - back, 1)
        mask = (group_of == j) & (jnp.broadcast_to(moved[8:9], (seqs, count)) == seq_at)
        for h in range(2 * j, min(2 * j + 2, heads)):
            level = jnp.where(mask, jnp.broadcast_to(moved[h : h + 1], (seqs, count)), GONE)
            best = jnp.max(level, axis=1, keepdims=True)
            share = jnp.exp(level - best)
            share = share / jnp.sum(share, axis=1, keepdims=True)
            shares.append(share.astype(BF16))
    mixed = jnp.dot(jnp.concatenate(shares, axis=0), both, preferred_element_type=F32)
    attention = jnp.concatenate(
        [
            mixed[h * seqs : (h + 1) * seqs, (h % 2) * head_dim : (h % 2 + 1) * head_dim].astype(BF16)
            for h in range(heads)
        ],
        axis=1,
    )
    w_load.wait()
    product = lax.dot_general(
        attention, wbuf[...], (((1,), (1,)), ((), ())), preferred_element_type=F32
    )
    share_rows = seqs // owners
    for x in range(owners):
        part[x] = product[x * share_rows : (x + 1) * share_rows].astype(BF16)

    def give(k):
        there = lax.rem(mine + k, owners)
        return remote(part.at[there], landed.at[k], p_send.at[k], p_recv.at[k], {"tensor": there})

    @pl.when(rank < owners - 1)
    def _():
        pl.semaphore_wait(met, owners - 1 - rank)

    for k in far_first(owners):
        give(k).start()
    result = part[mine].astype(F32)

    for k in range(1, owners):
        give(k).wait_recv()
        result = result + landed[k].astype(F32)
    out[...] = result.astype(BF16)

    q_drain()
    g_drain()

    for k in range(1, owners):
        give(k).wait_send()


def solution(mesh):
    chips = mesh.shape["seq"] // CORES
    owners = mesh.shape["tensor"]

    def local(query, key_cache, value_cache, alibi_slopes, block_seq, block_pos, lengths, out_weight):
        heads = alibi_slopes.shape[0]
        rows, features = query.shape
        blocks, block_len, _ = key_cache.shape
        seqs = lengths.shape[0]
        columns = out_weight.shape[1]
        head_dim = features // heads
        message = ((heads + 1) // 2 * blocks, 2 * head_dim)
        hbm = pl.BlockSpec(memory_space=pltpu.HBM)
        dma = pltpu.SemaphoreType.DMA
        return pl.pallas_call(
            functools.partial(kernel, chips, owners, heads),
            out_shape=pltpu.VMEM((seqs // owners, columns), BF16),
            in_specs=[hbm] * 8,
            out_specs=pl.BlockSpec(memory_space=pltpu.VMEM),
            scratch_shapes=[
                pltpu.SMEM(alibi_slopes.shape, F32),
                pltpu.SMEM(block_seq.shape, jnp.int32),
                pltpu.SMEM(block_pos.shape, jnp.int32),
                pltpu.SMEM(lengths.shape, jnp.int32),
                pltpu.VMEM(key_cache.shape, BF16),
                pltpu.VMEM((blocks, features, block_len), BF16),
                pltpu.VMEM(value_cache.shape, BF16),
                pltpu.VMEM(out_weight.shape[::-1], BF16),
                pltpu.VMEM((CORES * chips, rows, features), BF16),
                pltpu.VMEM((CORES, chips, *message), BF16),
                pltpu.VMEM((owners, seqs // owners, columns), BF16),
                pltpu.VMEM((owners, seqs // owners, columns), BF16),
                dma((8,)),
                pltpu.SemaphoreType.REGULAR,
                dma,
                dma,
                dma,
                dma,
                dma,
                dma((CORES * chips,)),
                dma,
                dma((chips,)),
                dma((2,)),
                dma((owners,)),
                dma((owners,)),
            ],
            compiler_params=pltpu.CompilerParams(
                collective_id=0, has_side_effects=True
            ),
        )(query, key_cache, value_cache, alibi_slopes, block_seq, block_pos, lengths, out_weight.T)

    placed = (
        P(("group", "seq"), "tensor"),
        P(("group", "seq"), None, "tensor"),
        P(("group", "seq"), None, "tensor"),
        P("tensor"),
        P(("group", "seq")),
        P(("group", "seq")),
        P("group"),
        P("tensor", "seq"),
    )
    return jax.shard_map(
        local, mesh=mesh, in_specs=placed, out_specs=P(("group", "tensor"), "seq"), check_vma=False
    )
```

```python
import functools
import math

import jax
import jax.numpy as jnp
from jax import lax
from jax.experimental import pallas as pl
from jax.experimental.pallas import tpu as pltpu
from jax.sharding import PartitionSpec as P

MESH = pl.DeviceIdType.MESH
F32 = jnp.float32
BF16 = jnp.bfloat16
CORES = 2
HUBS = (3, -3, 6, -6)
LATE = 3
GONE = -1e30


def remote(src, dst, send, recv, where):
    return pltpu.make_async_remote_copy(
        src_ref=src, dst_ref=dst, send_sem=send, recv_sem=recv, device_id=where, device_id_type=MESH
    )


def spread(slots, chips, z, c, send, recv, relay):
    partner = {"seq": z * CORES + 1 - c}

    def pass_on(place, step):
        there = lax.rem(z + chips + step, chips) * CORES + c
        at = (place + step) % chips
        sem = recv.at[HUBS.index(step)] if place == 0 and step in HUBS else recv.at[len(HUBS)]
        remote(slots.at[c, place % chips], slots.at[c, at], send, sem, {"seq": there}).start()

    def landed(at, sem):
        remote(slots.at[c, at], slots.at[c, at], send, sem, partner).wait_recv()

    direct = [step for step in range(-(chips // 2) + 1, chips // 2 + 1) if step in HUBS or abs(step) in (1, chips // 2)]
    for step in sorted(direct, key=lambda step: -abs(step)):
        pass_on(0, step)
    for i, hub in enumerate(HUBS):
        landed(hub % chips, recv.at[i])
        for step in (1, -1):
            pass_on(hub, step)
    landed(pl.ds(0, chips - 1 - len(HUBS)), recv.at[len(HUBS)])
    half = remote(slots.at[c], slots.at[c], relay.at[0], relay.at[1], partner)
    half.start()
    half.wait_recv()

    def drain():
        half.wait_send()
        every = pl.ds(0, chips - 1)
        remote(slots.at[c, every], slots.at[c, every], send, relay.at[1], partner).wait_send()

    return drain


def far_first(n):
    return sorted(range(1, n), key=lambda m: -min(m, n - m))


def kernel(
    chips, owners, heads,
    q_hbm, k_hbm, v_hbm, slopes_hbm, block_seq_hbm, block_pos_hbm, lengths_hbm, w_hbm, out,
    slopes, block_seq, block_pos, lengths, kbuf, kturn, vbuf, wbuf, qall, gall, part, landed,
    load, met, e_send, f_send, f_recv, e_recv, r_recv, d_recv, q_send, q_recv, g_send, g_recv, g_relay, p_send, p_recv,
):
    seq = lax.axis_index("seq")
    mine = lax.axis_index("tensor")
    devices = CORES * chips
    z, c = seq // CORES, lax.rem(seq, CORES)
    blocks, block_len, features = k_hbm.shape
    rows = q_hbm.shape[0]
    head_dim = features // heads
    seqs = lengths_hbm.shape[0]
    scale = 1.0 / math.sqrt(head_dim)

    order = sorted(range(owners), key=lambda x: (min(x, owners - x), x * 2 <= owners))
    order = order[:-3] + [owners // 2] + [x for x in order[-3:] if x * 2 != owners]
    rank = sum(jnp.where(mine == x, r, 0) for r, x in enumerate(order))

    first_late = chips - LATE

    barrier = pltpu.get_barrier_semaphore()

    def greet_seq(j, _):
        pl.semaphore_signal(barrier, inc=1, device_id={"seq": j}, device_id_type=MESH)
        return 0

    q_load = pltpu.make_async_copy(q_hbm, qall.at[seq], load.at[0])
    q_load.start()

    @pl.when(seq > 0)
    def _():
        lax.fori_loop(seq + 1, devices, greet_seq, 0)

    @pl.when(seq == 1)
    def _():
        greet_seq(0, 0)

    for r, x in enumerate(order):

        @pl.when(r > rank)
        def _(x=x):
            pl.semaphore_signal(barrier, inc=1, device_id={"tensor": x}, device_id_type=MESH)


    small = [
        pltpu.make_async_copy(src, dst, load.at[4 + i])
        for i, (src, dst) in enumerate(
            (
                (slopes_hbm, slopes),
                (block_seq_hbm, block_seq),
                (block_pos_hbm, block_pos),
                (lengths_hbm, lengths),
            )
        )
    ]
    k_load = pltpu.make_async_copy(k_hbm, kbuf, load.at[1])
    v_load = pltpu.make_async_copy(v_hbm, vbuf, load.at[2])
    w_load = pltpu.make_async_copy(w_hbm, wbuf, load.at[3])
    for copy in small:
        copy.start()
    k_load.start()
    v_load.start()
    w_load.start()
    q_load.wait()
    before = jnp.where(seq == 0, 1, seq - 1) + rank

    @pl.when(before > 0)
    def _():
        pl.semaphore_wait(barrier, before)

    def give_q(j):
        return remote(qall.at[seq], qall.at[seq], q_send, q_recv.at[seq], {"seq": j})

    def arrival(j):
        return remote(qall.at[j], qall.at[j], q_send, q_recv.at[j], {"seq": z * CORES + 1 - c})

    def several(slots, recv, j, send=q_send):
        return remote(qall.at[slots], qall.at[slots], send, recv, {"seq": j})

    pair = pl.ds(0, CORES)
    rest = pl.ds(1, devices - 1)

    def early(core):
        return pl.ds(core * first_late, first_late)

    def send_down(i, _):
        far = chips // 2
        step = (i + 1) // 2
        k = jnp.where(lax.rem(i, 2) == 0, far - step, far + step)
        for cc in range(CORES):
            j = lax.rem(z + k, chips) * CORES + cc

            @pl.when((j > 0) & (j < seq))
            def _():
                give_q(j).start()

        return 0

    lax.fori_loop(0, chips, send_down, 0)

    for r, x in enumerate(order):

        @pl.when(r < rank)
        def _(x=x):
            pl.semaphore_signal(met, inc=1, device_id={"tensor": x}, device_id_type=MESH)

    k_load.wait()
    for b in range(blocks):
        kturn[b] = kbuf[b].T

    def arrive(j, _):
        arrival(j).wait_recv()
        return 0

    @pl.when(seq == 0)
    def _():
        give_q(1).start()
        several(rest, r_recv, 1).wait_recv()

    @pl.when(seq == 1)
    def _():
        arrival(0).wait_recv()

        def pass_pair(j, _):
            arrival(j).wait_recv()
            several(pair, f_recv, j, f_send).start()
            return 0

        lax.fori_loop(CORES, first_late * CORES, pass_pair, 0)

        def pass_early(j, _):
            arrival(j).wait_recv()
            several(early(lax.rem(j, CORES)), e_recv, j, e_send.at[j - first_late * CORES]).start()
            return 0

        lax.fori_loop(first_late * CORES, devices, pass_early, 0)
        several(rest, r_recv, 0).start()

    @pl.when(seq > 1)
    def _():
        def send_up(j, _):
            arrival(j).wait_recv()

            @pl.when((j < first_late * CORES) | (z >= first_late))
            def _():
                give_q(j).start()

            return 0

        lax.fori_loop(seq + 1, devices, send_up, 0)

        @pl.when(z >= first_late)
        def _():
            several(early(c), e_recv, 1).wait_recv()
            several(early(c), d_recv, z * CORES + 1 - c, f_send).start()
            lax.fori_loop(first_late * CORES, seq, arrive, 0)
            several(early(1 - c), d_recv, 1).wait_recv()

        @pl.when(z < first_late)
        def _():
            several(pair, f_recv, 1).wait_recv()
            lax.fori_loop(CORES, seq, arrive, 0)

    def q_drain():
        @pl.when(seq == 0)
        def _():
            give_q(1).wait_send()

        @pl.when(seq == 1)
        def _():
            several(rest, r_recv, 0).wait_send()
            size = kbuf.at[0, pl.ds(0, (first_late - 1) * CORES * CORES * rows)]
            remote(size, size, f_send, r_recv, {"seq": 0}).wait_send()
            for i in range(LATE * CORES):
                several(early(0), e_recv, 0, e_send.at[i]).wait_send()

        @pl.when((seq > 1) & (z < first_late))
        def _():
            several(pl.ds(0, devices - 2 - LATE * CORES), r_recv, 1).wait_send()

        @pl.when(z >= first_late)
        def _():
            several(pl.ds(0, devices - 2), r_recv, 1).wait_send()
            several(early(c), r_recv, 1, f_send).wait_send()

    sub = lax.broadcasted_iota(jnp.int32, (8, features), 0)
    lane = lax.broadcasted_iota(jnp.int32, (8, features), 1)
    own_head = lane // head_dim == sub
    t_at = lax.broadcasted_iota(jnp.int32, (8, block_len), 1)
    h_at = lax.broadcasted_iota(jnp.int32, (8, block_len), 0)
    a_sub = lax.broadcasted_iota(jnp.int32, (8, head_dim), 0)
    a_lane = lax.broadcasted_iota(jnp.int32, (8, head_dim), 1)

    v_load.wait()
    for copy in small:
        copy.wait()
    slope = jnp.zeros((8, block_len), F32)
    for h in range(heads):
        slope = jnp.where(h_at == h, slopes[h], slope)
    wholes = []
    for b in range(blocks):
        s = block_seq[b]
        length = lengths[s]
        owner = s // rows
        r = lax.rem(s, rows)
        pair = qall[owner].astype(F32)
        row = pair[0:1]
        for i in range(1, rows):
            row = jnp.where(r == i, pair[i : i + 1], row)
        wide = jnp.where(own_head, jnp.broadcast_to(row, (8, features)), 0.0).astype(BF16)
        scores = lax.dot_general(
            wide, kturn[b], (((1,), (0,)), ((), ())), preferred_element_type=F32
        )
        placed = block_pos[b] * block_len + t_at
        live = placed < length
        distance = (length - 1 - placed).astype(F32)
        scores = jnp.where(live, scores * scale - slope * distance, GONE)
        top = jnp.max(scores, axis=1, keepdims=True)
        weights = jnp.where(live, jnp.exp(scores - top), 0.0)
        total = jnp.sum(weights, axis=1, keepdims=True)
        acc = jnp.dot(weights.astype(BF16), vbuf[b], preferred_element_type=F32)
        o = jnp.sum(jnp.where(own_head, acc / total, 0.0), axis=0, keepdims=True)
        lse = top + jnp.log(total)
        high = lse.astype(BF16).astype(F32)
        mid = (lse - high).astype(BF16).astype(F32)
        low = lse - high - mid
        tail = jnp.where(a_lane == a_sub, high, 0.0)
        tail = jnp.where(a_lane == a_sub + 8, mid, tail)
        tail = jnp.where(a_lane == a_sub + 16, low, tail)
        tail = jnp.where((a_lane == 24) & (a_sub == 0), s.astype(F32), tail)
        tail = jnp.sum(jnp.where(a_sub < heads, tail, 0.0), axis=0, keepdims=True)
        wholes.append(jnp.concatenate([o, tail], axis=1))

    wide = 2 * head_dim
    groups = (heads + 1) // 2
    m_sub = lax.broadcasted_iota(jnp.int32, (8, wide), 0)
    halves = []
    for first in range(0, groups * blocks, 8):
        half = jnp.zeros((8, wide), F32)
        for i in range(8):
            j, b = divmod(first + i, blocks)
            piece = wholes[b][:, j * wide : (j + 1) * wide]
            half = jnp.where(m_sub == i, jnp.broadcast_to(piece, (8, wide)), half)
        halves.append(half)
    gall[c, 0] = jnp.concatenate(halves, axis=0).astype(BF16)

    g_drain = spread(gall, chips, z, c, g_send, g_recv, g_relay)

    high_rows = groups * blocks
    count = CORES * chips * high_rows
    both = gall[...].reshape(count, wide)
    p_sub = lax.broadcasted_iota(jnp.int32, (16, head_dim), 0)
    p_lane = lax.broadcasted_iota(jnp.int32, (16, head_dim), 1)
    pick = (p_sub < 8) & (p_lane < 24) & (lax.rem(p_lane, 8) == p_sub)
    pick = pick | ((p_sub == 8) & (p_lane == 24))
    pick = jnp.where(pick, 1.0, 0.0).astype(BF16)
    tails = lax.dot_general(
        pick, both[:, head_dim:], (((1,), (1,)), ((), ())), preferred_element_type=F32
    )
    column = lax.broadcasted_iota(jnp.int32, (seqs, count), 1)
    group_of = lax.rem(column // blocks, groups)
    seq_at = lax.broadcasted_iota(jnp.int32, (seqs, count), 0).astype(F32)
    shares = []
    for j in range(groups):
        back = (groups - 1 - j) * blocks
        moved = tails if back == 0 else pltpu.roll(tails, count - back, 1)
        mask = (group_of == j) & (jnp.broadcast_to(moved[8:9], (seqs, count)) == seq_at)
        for h in range(2 * j, min(2 * j + 2, heads)):
            level = jnp.where(mask, jnp.broadcast_to(moved[h : h + 1], (seqs, count)), GONE)
            best = jnp.max(level, axis=1, keepdims=True)
            share = jnp.exp(level - best)
            share = share / jnp.sum(share, axis=1, keepdims=True)
            shares.append(share.astype(BF16))
    mixed = jnp.dot(jnp.concatenate(shares, axis=0), both, preferred_element_type=F32)
    attention = jnp.concatenate(
        [
            mixed[h * seqs : (h + 1) * seqs, (h % 2) * head_dim : (h % 2 + 1) * head_dim].astype(BF16)
            for h in range(heads)
        ],
        axis=1,
    )
    w_load.wait()
    product = lax.dot_general(
        attention, wbuf[...], (((1,), (1,)), ((), ())), preferred_element_type=F32
    )
    share_rows = seqs // owners
    for x in range(owners):
        part[x] = product[x * share_rows : (x + 1) * share_rows].astype(BF16)

    def give(k):
        there = lax.rem(mine + k, owners)
        return remote(part.at[there], landed.at[k - 1], p_send, p_recv, {"tensor": there})

    @pl.when(rank < owners - 1)
    def _():
        pl.semaphore_wait(met, owners - 1 - rank)

    for k in far_first(owners):
        give(k).start()
    result = part[mine].astype(F32)

    others = pl.ds(0, owners - 1)
    all_others = remote(part.at[others], landed.at[others], p_send, p_recv, {"tensor": mine})
    all_others.wait_recv()
    for k in range(1, owners):
        result = result + landed[k - 1].astype(F32)
    out[...] = result.astype(BF16)

    q_drain()
    g_drain()

    all_others.wait_send()


def solution(mesh):
    chips = mesh.shape["seq"] // CORES
    owners = mesh.shape["tensor"]

    def local(query, key_cache, value_cache, alibi_slopes, block_seq, block_pos, lengths, out_weight):
        heads = alibi_slopes.shape[0]
        rows, features = query.shape
        blocks, block_len, _ = key_cache.shape
        seqs = lengths.shape[0]
        columns = out_weight.shape[1]
        head_dim = features // heads
        message = ((heads + 1) // 2 * blocks, 2 * head_dim)
        hbm = pl.BlockSpec(memory_space=pltpu.HBM)
        dma = pltpu.SemaphoreType.DMA
        return pl.pallas_call(
            functools.partial(kernel, chips, owners, heads),
            out_shape=pltpu.VMEM((seqs // owners, columns), BF16),
            in_specs=[hbm] * 8,
            out_specs=pl.BlockSpec(memory_space=pltpu.VMEM),
            scratch_shapes=[
                pltpu.SMEM(alibi_slopes.shape, F32),
                pltpu.SMEM(block_seq.shape, jnp.int32),
                pltpu.SMEM(block_pos.shape, jnp.int32),
                pltpu.SMEM(lengths.shape, jnp.int32),
                pltpu.VMEM(key_cache.shape, BF16),
                pltpu.VMEM((blocks, features, block_len), BF16),
                pltpu.VMEM(value_cache.shape, BF16),
                pltpu.VMEM(out_weight.shape[::-1], BF16),
                pltpu.VMEM((CORES * chips, rows, features), BF16),
                pltpu.VMEM((CORES, chips, *message), BF16),
                pltpu.VMEM((owners, seqs // owners, columns), BF16),
                pltpu.VMEM((owners, seqs // owners, columns), BF16),
                dma((8,)),
                pltpu.SemaphoreType.REGULAR,
                dma((LATE * CORES,)),
                dma,
                dma,
                dma,
                dma,
                dma,
                dma,
                dma((CORES * chips,)),
                dma,
                dma((len(HUBS) + 1,)),
                dma((2,)),
                dma,
                dma,
            ],
            compiler_params=pltpu.CompilerParams(
                collective_id=0, has_side_effects=True
            ),
        )(query, key_cache, value_cache, alibi_slopes, block_seq, block_pos, lengths, out_weight.T)

    placed = (
        P(("group", "seq"), "tensor"),
        P(("group", "seq"), None, "tensor"),
        P(("group", "seq"), None, "tensor"),
        P("tensor"),
        P(("group", "seq")),
        P(("group", "seq")),
        P("group"),
        P("tensor", "seq"),
    )
    return jax.shard_map(
        local, mesh=mesh, in_specs=placed, out_specs=P(("group", "tensor"), "seq"), check_vma=False
    )
```

```python
import functools
import math

import jax
import jax.numpy as jnp
from jax import lax
from jax.experimental import pallas as pl
from jax.experimental.pallas import tpu as pltpu
from jax.sharding import PartitionSpec as P

MESH = pl.DeviceIdType.MESH
F32 = jnp.float32
BF16 = jnp.bfloat16
CORES = 2
LATE = 3
GONE = -1e30


def remote(src, dst, send, recv, where):
    return pltpu.make_async_remote_copy(
        src_ref=src, dst_ref=dst, send_sem=send, recv_sem=recv, device_id=where, device_id_type=MESH
    )


def spread(slots, chips, z, c, send, recv, relay):
    partner = {"seq": z * CORES + 1 - c}
    for k in far_first(chips):
        there = lax.rem(z + k, chips) * CORES + c
        remote(slots.at[c, 0], slots.at[c, k], send, recv.at[0], {"seq": there}).start()
    every = pl.ds(0, chips - 1)
    remote(slots.at[c, every], slots.at[c, every], send, recv.at[0], partner).wait_recv()
    half = remote(slots.at[c], slots.at[c], relay.at[0], relay.at[1], partner)
    half.start()
    half.wait_recv()

    def drain():
        half.wait_send()
        remote(slots.at[c, every], slots.at[c, every], send, relay.at[1], partner).wait_send()

    return drain


def far_first(n):
    return sorted(range(1, n), key=lambda m: -min(m, n - m))


def kernel(
    chips, owners, heads,
    q_hbm, k_hbm, v_hbm, slopes_hbm, block_seq_hbm, block_pos_hbm, lengths_hbm, w_hbm, out,
    slopes, block_seq, block_pos, lengths, kbuf, kturn, vbuf, wbuf, qall, gall, part, landed,
    load, met, ready, e_send, f_send, f_recv, e_recv, r_recv, d_recv, q_send, q_recv, g_send, g_recv, g_relay, p_send, p_recv,
):
    seq = lax.axis_index("seq")
    mine = lax.axis_index("tensor")
    devices = CORES * chips
    z, c = seq // CORES, lax.rem(seq, CORES)
    blocks, block_len, features = k_hbm.shape
    rows = q_hbm.shape[0]
    head_dim = features // heads
    seqs = lengths_hbm.shape[0]
    scale = 1.0 / math.sqrt(head_dim)

    order = sorted(range(owners), key=lambda x: (min(x, owners - x), x * 2 <= owners))
    order = order[:-3] + [owners // 2] + [x for x in order[-3:] if x * 2 != owners]
    rank = sum(jnp.where(mine == x, r, 0) for r, x in enumerate(order))

    first_late = chips - LATE

    barrier = pltpu.get_barrier_semaphore()

    def greet_seq(j, _):
        pl.semaphore_signal(barrier, inc=1, device_id={"seq": j}, device_id_type=MESH)
        return 0

    q_load = pltpu.make_async_copy(q_hbm, qall.at[seq], load.at[0])
    q_load.start()

    @pl.when(seq > 0)
    def _():
        lax.fori_loop(seq + 1, devices, greet_seq, 0)

    @pl.when(seq == 1)
    def _():
        greet_seq(0, 0)

    for r, x in enumerate(order):

        @pl.when((r > rank) & (seq == 1))
        def _(x=x):
            pl.semaphore_signal(barrier, inc=1, device_id={"tensor": x}, device_id_type=MESH)


    small = [
        pltpu.make_async_copy(src, dst, load.at[4 + i])
        for i, (src, dst) in enumerate(
            (
                (slopes_hbm, slopes),
                (block_seq_hbm, block_seq),
                (block_pos_hbm, block_pos),
                (lengths_hbm, lengths),
            )
        )
    ]
    k_load = pltpu.make_async_copy(k_hbm, kbuf, load.at[1])
    v_load = pltpu.make_async_copy(v_hbm, vbuf, load.at[2])
    w_load = pltpu.make_async_copy(w_hbm, wbuf, load.at[3])
    for copy in small:
        copy.start()
    k_load.start()
    v_load.start()
    w_load.start()
    q_load.wait()
    before = jnp.where(seq == 0, 1, jnp.where(seq == 1, rank, seq - 1))

    @pl.when(before > 0)
    def _():
        pl.semaphore_wait(barrier, before)

    def give_q(j):
        return remote(qall.at[seq], qall.at[seq], q_send, q_recv.at[seq], {"seq": j})

    def arrival(j):
        return remote(qall.at[j], qall.at[j], q_send, q_recv.at[j], {"seq": z * CORES + 1 - c})

    def several(slots, recv, j, send=q_send):
        return remote(qall.at[slots], qall.at[slots], send, recv, {"seq": j})

    pair = pl.ds(0, CORES)
    rest = pl.ds(1, devices - 1)

    def early(core):
        return pl.ds(core * first_late, first_late)

    def send_down(i, _):
        far = chips // 2
        step = (i + 1) // 2
        k = jnp.where(lax.rem(i, 2) == 0, far - step, far + step)
        for cc in range(CORES):
            j = lax.rem(z + k, chips) * CORES + cc

            @pl.when((j > 0) & (j < seq))
            def _():
                give_q(j).start()

        return 0

    lax.fori_loop(0, chips, send_down, 0)

    for r, x in enumerate(order):

        @pl.when((r < rank) & (seq == 1))
        def _(x=x):
            pl.semaphore_signal(met, inc=1, device_id={"tensor": x}, device_id_type=MESH)

    k_load.wait()
    for b in range(blocks):
        kturn[b] = kbuf[b].T

    def arrive(j, _):
        arrival(j).wait_recv()
        return 0

    @pl.when(seq == 0)
    def _():
        give_q(1).start()
        several(rest, r_recv, 1).wait_recv()

    @pl.when(seq == 1)
    def _():
        arrival(0).wait_recv()

        def pass_pair(j, _):
            arrival(j).wait_recv()
            several(pair, f_recv, j, f_send).start()
            return 0

        lax.fori_loop(CORES, first_late * CORES, pass_pair, 0)

        def pass_early(j, _):
            arrival(j).wait_recv()
            several(early(lax.rem(j, CORES)), e_recv, j, e_send.at[j - first_late * CORES]).start()
            return 0

        lax.fori_loop(first_late * CORES, devices, pass_early, 0)
        several(rest, r_recv, 0).start()

        @pl.when(rank < owners - 1)
        def _():
            pl.semaphore_wait(met, owners - 1 - rank)

        for step in range(1, owners):
            there = {"tensor": lax.rem(mine + step, owners)}
            pl.semaphore_signal(ready, inc=1, device_id=there, device_id_type=MESH)


    @pl.when(seq > 1)
    def _():
        def send_up(j, _):
            arrival(j).wait_recv()

            @pl.when((j < first_late * CORES) | (z >= first_late))
            def _():
                give_q(j).start()

            return 0

        lax.fori_loop(seq + 1, devices, send_up, 0)

        @pl.when(z >= first_late)
        def _():
            several(early(c), e_recv, 1).wait_recv()
            several(early(c), d_recv, z * CORES + 1 - c, f_send).start()
            lax.fori_loop(first_late * CORES, seq, arrive, 0)
            several(early(1 - c), d_recv, 1).wait_recv()

        @pl.when(z < first_late)
        def _():
            several(pair, f_recv, 1).wait_recv()
            lax.fori_loop(CORES, seq, arrive, 0)

    def q_drain():
        @pl.when(seq == 0)
        def _():
            give_q(1).wait_send()

        @pl.when(seq == 1)
        def _():
            several(rest, r_recv, 0).wait_send()
            size = kbuf.at[0, pl.ds(0, (first_late - 1) * CORES * CORES * rows)]
            remote(size, size, f_send, r_recv, {"seq": 0}).wait_send()
            for i in range(LATE * CORES):
                several(early(0), e_recv, 0, e_send.at[i]).wait_send()

        @pl.when((seq > 1) & (z < first_late))
        def _():
            several(pl.ds(0, devices - 2 - LATE * CORES), r_recv, 1).wait_send()

        @pl.when(z >= first_late)
        def _():
            several(pl.ds(0, devices - 2), r_recv, 1).wait_send()
            several(early(c), r_recv, 1, f_send).wait_send()

    sub = lax.broadcasted_iota(jnp.int32, (8, features), 0)
    lane = lax.broadcasted_iota(jnp.int32, (8, features), 1)
    own_head = lane // head_dim == sub
    t_at = lax.broadcasted_iota(jnp.int32, (8, block_len), 1)
    h_at = lax.broadcasted_iota(jnp.int32, (8, block_len), 0)
    a_sub = lax.broadcasted_iota(jnp.int32, (8, head_dim), 0)
    a_lane = lax.broadcasted_iota(jnp.int32, (8, head_dim), 1)

    v_load.wait()
    for copy in small:
        copy.wait()
    slope = jnp.zeros((8, block_len), F32)
    for h in range(heads):
        slope = jnp.where(h_at == h, slopes[h], slope)
    wholes = []
    for b in range(blocks):
        s = block_seq[b]
        length = lengths[s]
        owner = s // rows
        r = lax.rem(s, rows)
        pair = qall[owner].astype(F32)
        row = pair[0:1]
        for i in range(1, rows):
            row = jnp.where(r == i, pair[i : i + 1], row)
        wide = jnp.where(own_head, jnp.broadcast_to(row, (8, features)), 0.0).astype(BF16)
        scores = lax.dot_general(
            wide, kturn[b], (((1,), (0,)), ((), ())), preferred_element_type=F32
        )
        placed = block_pos[b] * block_len + t_at
        live = placed < length
        distance = (length - 1 - placed).astype(F32)
        scores = jnp.where(live, scores * scale - slope * distance, GONE)
        top = jnp.max(scores, axis=1, keepdims=True)
        weights = jnp.where(live, jnp.exp(scores - top), 0.0)
        total = jnp.sum(weights, axis=1, keepdims=True)
        acc = jnp.dot(weights.astype(BF16), vbuf[b], preferred_element_type=F32)
        o = jnp.sum(jnp.where(own_head, acc / total, 0.0), axis=0, keepdims=True)
        lse = top + jnp.log(total)
        high = lse.astype(BF16).astype(F32)
        mid = (lse - high).astype(BF16).astype(F32)
        low = lse - high - mid
        tail = jnp.where(a_lane == a_sub, high, 0.0)
        tail = jnp.where(a_lane == a_sub + 8, mid, tail)
        tail = jnp.where(a_lane == a_sub + 16, low, tail)
        tail = jnp.where((a_lane == 24) & (a_sub == 0), s.astype(F32), tail)
        tail = jnp.sum(jnp.where(a_sub < heads, tail, 0.0), axis=0, keepdims=True)
        wholes.append(jnp.concatenate([o, tail], axis=1))

    wide = 2 * head_dim
    groups = (heads + 1) // 2
    m_sub = lax.broadcasted_iota(jnp.int32, (8, wide), 0)
    halves = []
    for first in range(0, groups * blocks, 8):
        half = jnp.zeros((8, wide), F32)
        for i in range(8):
            j, b = divmod(first + i, blocks)
            piece = wholes[b][:, j * wide : (j + 1) * wide]
            half = jnp.where(m_sub == i, jnp.broadcast_to(piece, (8, wide)), half)
        halves.append(half)
    gall[c, 0] = jnp.concatenate(halves, axis=0).astype(BF16)

    @pl.when(seq == 1)
    def _():
        pl.semaphore_wait(ready, owners - 1)

    g_drain = spread(gall, chips, z, c, g_send, g_recv, g_relay)

    high_rows = groups * blocks
    count = CORES * chips * high_rows
    both = gall[...].reshape(count, wide)
    p_sub = lax.broadcasted_iota(jnp.int32, (16, head_dim), 0)
    p_lane = lax.broadcasted_iota(jnp.int32, (16, head_dim), 1)
    pick = (p_sub < 8) & (p_lane < 24) & (lax.rem(p_lane, 8) == p_sub)
    pick = pick | ((p_sub == 8) & (p_lane == 24))
    pick = jnp.where(pick, 1.0, 0.0).astype(BF16)
    tails = lax.dot_general(
        pick, both[:, head_dim:], (((1,), (1,)), ((), ())), preferred_element_type=F32
    )
    column = lax.broadcasted_iota(jnp.int32, (seqs, count), 1)
    group_of = lax.rem(column // blocks, groups)
    seq_at = lax.broadcasted_iota(jnp.int32, (seqs, count), 0).astype(F32)
    shares = []
    for j in range(groups):
        back = (groups - 1 - j) * blocks
        moved = tails if back == 0 else pltpu.roll(tails, count - back, 1)
        mask = (group_of == j) & (jnp.broadcast_to(moved[8:9], (seqs, count)) == seq_at)
        for h in range(2 * j, min(2 * j + 2, heads)):
            level = jnp.where(mask, jnp.broadcast_to(moved[h : h + 1], (seqs, count)), GONE)
            best = jnp.max(level, axis=1, keepdims=True)
            share = jnp.exp(level - best)
            share = share / jnp.sum(share, axis=1, keepdims=True)
            shares.append(share.astype(BF16))
    mixed = jnp.dot(jnp.concatenate(shares, axis=0), both, preferred_element_type=F32)
    attention = jnp.concatenate(
        [
            mixed[h * seqs : (h + 1) * seqs, (h % 2) * head_dim : (h % 2 + 1) * head_dim].astype(BF16)
            for h in range(heads)
        ],
        axis=1,
    )
    w_load.wait()
    product = lax.dot_general(
        attention, wbuf[...], (((1,), (1,)), ((), ())), preferred_element_type=F32
    )
    share_rows = seqs // owners
    for x in range(owners):
        part[x] = product[x * share_rows : (x + 1) * share_rows].astype(BF16)

    def give(k):
        there = lax.rem(mine + k, owners)
        return remote(part.at[there], landed.at[k - 1], p_send, p_recv, {"tensor": there})

    for k in far_first(owners):
        give(k).start()
    result = part[mine].astype(F32)

    others = pl.ds(0, owners - 1)
    all_others = remote(part.at[others], landed.at[others], p_send, p_recv, {"tensor": mine})
    all_others.wait_recv()
    for k in range(1, owners):
        result = result + landed[k - 1].astype(F32)
    out[...] = result.astype(BF16)

    q_drain()
    g_drain()

    all_others.wait_send()


def solution(mesh):
    chips = mesh.shape["seq"] // CORES
    owners = mesh.shape["tensor"]

    def local(query, key_cache, value_cache, alibi_slopes, block_seq, block_pos, lengths, out_weight):
        heads = alibi_slopes.shape[0]
        rows, features = query.shape
        blocks, block_len, _ = key_cache.shape
        seqs = lengths.shape[0]
        columns = out_weight.shape[1]
        head_dim = features // heads
        message = ((heads + 1) // 2 * blocks, 2 * head_dim)
        hbm = pl.BlockSpec(memory_space=pltpu.HBM)
        dma = pltpu.SemaphoreType.DMA
        return pl.pallas_call(
            functools.partial(kernel, chips, owners, heads),
            out_shape=pltpu.VMEM((seqs // owners, columns), BF16),
            in_specs=[hbm] * 8,
            out_specs=pl.BlockSpec(memory_space=pltpu.VMEM),
            scratch_shapes=[
                pltpu.SMEM(alibi_slopes.shape, F32),
                pltpu.SMEM(block_seq.shape, jnp.int32),
                pltpu.SMEM(block_pos.shape, jnp.int32),
                pltpu.SMEM(lengths.shape, jnp.int32),
                pltpu.VMEM(key_cache.shape, BF16),
                pltpu.VMEM((blocks, features, block_len), BF16),
                pltpu.VMEM(value_cache.shape, BF16),
                pltpu.VMEM(out_weight.shape[::-1], BF16),
                pltpu.VMEM((CORES * chips, rows, features), BF16),
                pltpu.VMEM((CORES, chips, *message), BF16),
                pltpu.VMEM((owners, seqs // owners, columns), BF16),
                pltpu.VMEM((owners, seqs // owners, columns), BF16),
                dma((8,)),
                pltpu.SemaphoreType.REGULAR,
                pltpu.SemaphoreType.REGULAR,
                dma((LATE * CORES,)),
                dma,
                dma,
                dma,
                dma,
                dma,
                dma,
                dma((CORES * chips,)),
                dma,
                dma((1,)),
                dma((2,)),
                dma,
                dma,
            ],
            compiler_params=pltpu.CompilerParams(
                collective_id=0, has_side_effects=True
            ),
        )(query, key_cache, value_cache, alibi_slopes, block_seq, block_pos, lengths, out_weight.T)

    placed = (
        P(("group", "seq"), "tensor"),
        P(("group", "seq"), None, "tensor"),
        P(("group", "seq"), None, "tensor"),
        P("tensor"),
        P(("group", "seq")),
        P(("group", "seq")),
        P("group"),
        P("tensor", "seq"),
    )
    return jax.shard_map(
        local, mesh=mesh, in_specs=placed, out_specs=P(("group", "tensor"), "seq"), check_vma=False
    )
```

```python
import functools
import math

import jax
import jax.numpy as jnp
from jax import lax
from jax.experimental import pallas as pl
from jax.experimental.pallas import tpu as pltpu
from jax.sharding import PartitionSpec as P

MESH = pl.DeviceIdType.MESH
F32 = jnp.float32
BF16 = jnp.bfloat16
CORES = 2
LATE = 3
GONE = -1e30


def remote(src, dst, send, recv, where):
    return pltpu.make_async_remote_copy(
        src_ref=src, dst_ref=dst, send_sem=send, recv_sem=recv, device_id=where, device_id_type=MESH
    )


def spread(slots, chips, z, c, send, recv, relay):
    partner = {"seq": z * CORES + 1 - c}
    for chip in range(chips):

        @pl.when(chip != z)
        def _():
            behind = lax.rem(chip - z + chips, chips)
            there = {"seq": chip * CORES + c}
            remote(slots.at[c, 0], slots.at[c, behind], send, recv.at[0], there).start()

    every = pl.ds(0, chips - 1)
    remote(slots.at[c, every], slots.at[c, every], send, recv.at[0], partner).wait_recv()
    half = remote(slots.at[c], slots.at[c], relay.at[0], relay.at[1], partner)
    half.start()
    half.wait_recv()

    def drain():
        half.wait_send()
        remote(slots.at[c, every], slots.at[c, every], send, relay.at[1], partner).wait_send()

    return drain


def far_first(n):
    return sorted(range(1, n), key=lambda m: -min(m, n - m))


def kernel(
    chips, owners, heads,
    q_hbm, k_hbm, v_hbm, slopes_hbm, block_seq_hbm, block_pos_hbm, lengths_hbm, w_hbm, out,
    slopes, block_seq, block_pos, lengths, kbuf, kturn, vbuf, wbuf, qall, gall, part, landed,
    load, met, ready, e_send, f_send, f_recv, e_recv, r_recv, d_recv, q_send, q_recv, g_send, g_recv, g_relay, p_send, p_recv,
):
    seq = lax.axis_index("seq")
    mine = lax.axis_index("tensor")
    devices = CORES * chips
    z, c = seq // CORES, lax.rem(seq, CORES)
    blocks, block_len, features = k_hbm.shape
    rows = q_hbm.shape[0]
    head_dim = features // heads
    seqs = lengths_hbm.shape[0]
    scale = 1.0 / math.sqrt(head_dim)

    order = sorted(range(owners), key=lambda x: (min(x, owners - x), x * 2 <= owners))
    order = order[:-3] + [owners // 2] + [x for x in order[-3:] if x * 2 != owners]
    rank = sum(jnp.where(mine == x, r, 0) for r, x in enumerate(order))

    first_late = chips - LATE

    barrier = pltpu.get_barrier_semaphore()

    def greet_seq(j, _):
        pl.semaphore_signal(barrier, inc=1, device_id={"seq": j}, device_id_type=MESH)
        return 0

    q_load = pltpu.make_async_copy(q_hbm, qall.at[seq], load.at[0])
    q_load.start()

    @pl.when(seq > 0)
    def _():
        lax.fori_loop(seq + 1, devices, greet_seq, 0)

    @pl.when(seq == 1)
    def _():
        greet_seq(0, 0)

    for r, x in enumerate(order):

        @pl.when((r > rank) & (seq == 1))
        def _(x=x):
            pl.semaphore_signal(barrier, inc=1, device_id={"tensor": x}, device_id_type=MESH)


    small = [
        pltpu.make_async_copy(src, dst, load.at[4 + i])
        for i, (src, dst) in enumerate(
            (
                (slopes_hbm, slopes),
                (block_seq_hbm, block_seq),
                (block_pos_hbm, block_pos),
                (lengths_hbm, lengths),
            )
        )
    ]
    k_load = pltpu.make_async_copy(k_hbm, kbuf, load.at[1])
    v_load = pltpu.make_async_copy(v_hbm, vbuf, load.at[2])
    w_load = pltpu.make_async_copy(w_hbm, wbuf, load.at[3])
    for copy in small:
        copy.start()
    k_load.start()
    v_load.start()
    w_load.start()
    q_load.wait()
    before = jnp.where(seq == 0, 1, jnp.where(seq == 1, rank, seq - 1))

    @pl.when(before > 0)
    def _():
        pl.semaphore_wait(barrier, before)

    def give_q(j):
        return remote(qall.at[seq], qall.at[seq], q_send, q_recv.at[seq], {"seq": j})

    def arrival(j):
        return remote(qall.at[j], qall.at[j], q_send, q_recv.at[j], {"seq": z * CORES + 1 - c})

    def several(slots, recv, j, send=q_send):
        return remote(qall.at[slots], qall.at[slots], send, recv, {"seq": j})

    pair = pl.ds(0, CORES)
    rest = pl.ds(1, devices - 1)

    def early(core):
        return pl.ds(core * first_late, first_late)

    def send_down(i, _):
        far = chips // 2
        step = (i + 1) // 2
        k = jnp.where(lax.rem(i, 2) == 0, far - step, far + step)
        for cc in range(CORES):
            j = lax.rem(z + k, chips) * CORES + cc

            @pl.when((j > 0) & (j < seq))
            def _():
                give_q(j).start()

        return 0

    lax.fori_loop(0, chips, send_down, 0)

    for r, x in enumerate(order):

        @pl.when((r < rank) & (seq == 1))
        def _(x=x):
            pl.semaphore_signal(met, inc=1, device_id={"tensor": x}, device_id_type=MESH)

    k_load.wait()
    for b in range(blocks):
        kturn[b] = kbuf[b].T

    def arrive(j, _):
        arrival(j).wait_recv()
        return 0

    @pl.when(seq == 0)
    def _():
        give_q(1).start()
        several(rest, r_recv, 1).wait_recv()

    @pl.when(seq == 1)
    def _():
        arrival(0).wait_recv()

        def pass_pair(j, _):
            arrival(j).wait_recv()
            several(pair, f_recv, j, f_send).start()
            return 0

        lax.fori_loop(CORES, first_late * CORES, pass_pair, 0)

        def pass_early(j, _):
            arrival(j).wait_recv()
            several(early(lax.rem(j, CORES)), e_recv, j, e_send.at[j - first_late * CORES]).start()
            return 0

        lax.fori_loop(first_late * CORES, devices, pass_early, 0)
        several(rest, r_recv, 0).start()

        @pl.when(rank < owners - 1)
        def _():
            pl.semaphore_wait(met, owners - 1 - rank)

        for step in range(1, owners):
            there = {"tensor": lax.rem(mine + step, owners)}
            pl.semaphore_signal(ready, inc=1, device_id=there, device_id_type=MESH)


    @pl.when(seq > 1)
    def _():
        def send_up(j, _):
            arrival(j).wait_recv()

            @pl.when((j < first_late * CORES) | (z >= first_late))
            def _():
                give_q(j).start()

            return 0

        lax.fori_loop(seq + 1, devices, send_up, 0)

        @pl.when(z >= first_late)
        def _():
            several(early(c), e_recv, 1).wait_recv()
            several(early(c), d_recv, z * CORES + 1 - c, f_send).start()
            lax.fori_loop(first_late * CORES, seq, arrive, 0)
            several(early(1 - c), d_recv, 1).wait_recv()

        @pl.when(z < first_late)
        def _():
            several(pair, f_recv, 1).wait_recv()
            lax.fori_loop(CORES, seq, arrive, 0)

    def q_drain():
        @pl.when(seq == 0)
        def _():
            give_q(1).wait_send()

        @pl.when(seq == 1)
        def _():
            several(rest, r_recv, 0).wait_send()
            size = kbuf.at[0, pl.ds(0, (first_late - 1) * CORES * CORES * rows)]
            remote(size, size, f_send, r_recv, {"seq": 0}).wait_send()
            for i in range(LATE * CORES):
                several(early(0), e_recv, 0, e_send.at[i]).wait_send()

        @pl.when((seq > 1) & (z < first_late))
        def _():
            several(pl.ds(0, devices - 2 - LATE * CORES), r_recv, 1).wait_send()

        @pl.when(z >= first_late)
        def _():
            several(pl.ds(0, devices - 2), r_recv, 1).wait_send()
            several(early(c), r_recv, 1, f_send).wait_send()

    sub = lax.broadcasted_iota(jnp.int32, (8, features), 0)
    lane = lax.broadcasted_iota(jnp.int32, (8, features), 1)
    own_head = lane // head_dim == sub
    t_at = lax.broadcasted_iota(jnp.int32, (8, block_len), 1)
    h_at = lax.broadcasted_iota(jnp.int32, (8, block_len), 0)
    a_sub = lax.broadcasted_iota(jnp.int32, (8, head_dim), 0)
    a_lane = lax.broadcasted_iota(jnp.int32, (8, head_dim), 1)

    v_load.wait()
    for copy in small:
        copy.wait()
    slope = jnp.zeros((8, block_len), F32)
    for h in range(heads):
        slope = jnp.where(h_at == h, slopes[h], slope)
    wholes = []
    for b in range(blocks):
        s = block_seq[b]
        length = lengths[s]
        owner = s // rows
        r = lax.rem(s, rows)
        pair = qall[owner].astype(F32)
        row = pair[0:1]
        for i in range(1, rows):
            row = jnp.where(r == i, pair[i : i + 1], row)
        wide = jnp.where(own_head, jnp.broadcast_to(row, (8, features)), 0.0).astype(BF16)
        scores = lax.dot_general(
            wide, kturn[b], (((1,), (0,)), ((), ())), preferred_element_type=F32
        )
        placed = block_pos[b] * block_len + t_at
        live = placed < length
        distance = (length - 1 - placed).astype(F32)
        scores = jnp.where(live, scores * scale - slope * distance, GONE)
        top = jnp.max(scores, axis=1, keepdims=True)
        weights = jnp.where(live, jnp.exp(scores - top), 0.0)
        total = jnp.sum(weights, axis=1, keepdims=True)
        acc = jnp.dot(weights.astype(BF16), vbuf[b], preferred_element_type=F32)
        o = jnp.sum(jnp.where(own_head, acc / total, 0.0), axis=0, keepdims=True)
        lse = top + jnp.log(total)
        high = lse.astype(BF16).astype(F32)
        mid = (lse - high).astype(BF16).astype(F32)
        low = lse - high - mid
        tail = jnp.where(a_lane == a_sub, high, 0.0)
        tail = jnp.where(a_lane == a_sub + 8, mid, tail)
        tail = jnp.where(a_lane == a_sub + 16, low, tail)
        tail = jnp.where((a_lane == 24) & (a_sub == 0), s.astype(F32), tail)
        tail = jnp.sum(jnp.where(a_sub < heads, tail, 0.0), axis=0, keepdims=True)
        wholes.append(jnp.concatenate([o, tail], axis=1))

    wide = 2 * head_dim
    groups = (heads + 1) // 2
    m_sub = lax.broadcasted_iota(jnp.int32, (8, wide), 0)
    halves = []
    for first in range(0, groups * blocks, 8):
        half = jnp.zeros((8, wide), F32)
        for i in range(8):
            j, b = divmod(first + i, blocks)
            piece = wholes[b][:, j * wide : (j + 1) * wide]
            half = jnp.where(m_sub == i, jnp.broadcast_to(piece, (8, wide)), half)
        halves.append(half)
    gall[c, 0] = jnp.concatenate(halves, axis=0).astype(BF16)

    @pl.when(seq == 1)
    def _():
        pl.semaphore_wait(ready, owners - 1)

    g_drain = spread(gall, chips, z, c, g_send, g_recv, g_relay)

    high_rows = groups * blocks
    count = CORES * chips * high_rows
    both = gall[...].reshape(count, wide)
    p_sub = lax.broadcasted_iota(jnp.int32, (16, head_dim), 0)
    p_lane = lax.broadcasted_iota(jnp.int32, (16, head_dim), 1)
    pick = (p_sub < 8) & (p_lane < 24) & (lax.rem(p_lane, 8) == p_sub)
    pick = pick | ((p_sub == 8) & (p_lane == 24))
    pick = jnp.where(pick, 1.0, 0.0).astype(BF16)
    tails = lax.dot_general(
        pick, both[:, head_dim:], (((1,), (1,)), ((), ())), preferred_element_type=F32
    )
    column = lax.broadcasted_iota(jnp.int32, (seqs, count), 1)
    group_of = lax.rem(column // blocks, groups)
    seq_at = lax.broadcasted_iota(jnp.int32, (seqs, count), 0).astype(F32)
    shares = []
    for j in range(groups):
        back = (groups - 1 - j) * blocks
        moved = tails if back == 0 else pltpu.roll(tails, count - back, 1)
        mask = (group_of == j) & (jnp.broadcast_to(moved[8:9], (seqs, count)) == seq_at)
        for h in range(2 * j, min(2 * j + 2, heads)):
            level = jnp.where(mask, jnp.broadcast_to(moved[h : h + 1], (seqs, count)), GONE)
            best = jnp.max(level, axis=1, keepdims=True)
            share = jnp.exp(level - best)
            share = share / jnp.sum(share, axis=1, keepdims=True)
            shares.append(share.astype(BF16))
    mixed = jnp.dot(jnp.concatenate(shares, axis=0), both, preferred_element_type=F32)
    attention = jnp.concatenate(
        [
            mixed[h * seqs : (h + 1) * seqs, (h % 2) * head_dim : (h % 2 + 1) * head_dim].astype(BF16)
            for h in range(heads)
        ],
        axis=1,
    )
    w_load.wait()
    product = lax.dot_general(
        attention, wbuf[...], (((1,), (1,)), ((), ())), preferred_element_type=F32
    )
    share_rows = seqs // owners
    for x in range(owners):
        part[x] = product[x * share_rows : (x + 1) * share_rows].astype(BF16)

    def give(k):
        there = lax.rem(mine + k, owners)
        return remote(part.at[there], landed.at[k - 1], p_send, p_recv, {"tensor": there})

    for k in far_first(owners):
        give(k).start()
    result = part[mine].astype(F32)

    others = pl.ds(0, owners - 1)
    all_others = remote(part.at[others], landed.at[others], p_send, p_recv, {"tensor": mine})
    all_others.wait_recv()
    for k in range(1, owners):
        result = result + landed[k - 1].astype(F32)
    out[...] = result.astype(BF16)

    q_drain()
    g_drain()

    all_others.wait_send()


def solution(mesh):
    chips = mesh.shape["seq"] // CORES
    owners = mesh.shape["tensor"]

    def local(query, key_cache, value_cache, alibi_slopes, block_seq, block_pos, lengths, out_weight):
        heads = alibi_slopes.shape[0]
        rows, features = query.shape
        blocks, block_len, _ = key_cache.shape
        seqs = lengths.shape[0]
        columns = out_weight.shape[1]
        head_dim = features // heads
        message = ((heads + 1) // 2 * blocks, 2 * head_dim)
        hbm = pl.BlockSpec(memory_space=pltpu.HBM)
        dma = pltpu.SemaphoreType.DMA
        return pl.pallas_call(
            functools.partial(kernel, chips, owners, heads),
            out_shape=pltpu.VMEM((seqs // owners, columns), BF16),
            in_specs=[hbm] * 8,
            out_specs=pl.BlockSpec(memory_space=pltpu.VMEM),
            scratch_shapes=[
                pltpu.SMEM(alibi_slopes.shape, F32),
                pltpu.SMEM(block_seq.shape, jnp.int32),
                pltpu.SMEM(block_pos.shape, jnp.int32),
                pltpu.SMEM(lengths.shape, jnp.int32),
                pltpu.VMEM(key_cache.shape, BF16),
                pltpu.VMEM((blocks, features, block_len), BF16),
                pltpu.VMEM(value_cache.shape, BF16),
                pltpu.VMEM(out_weight.shape[::-1], BF16),
                pltpu.VMEM((CORES * chips, rows, features), BF16),
                pltpu.VMEM((CORES, chips, *message), BF16),
                pltpu.VMEM((owners, seqs // owners, columns), BF16),
                pltpu.VMEM((owners, seqs // owners, columns), BF16),
                dma((8,)),
                pltpu.SemaphoreType.REGULAR,
                pltpu.SemaphoreType.REGULAR,
                dma((LATE * CORES,)),
                dma,
                dma,
                dma,
                dma,
                dma,
                dma,
                dma((CORES * chips,)),
                dma,
                dma((1,)),
                dma((2,)),
                dma,
                dma,
            ],
            compiler_params=pltpu.CompilerParams(
                collective_id=0, has_side_effects=True
            ),
        )(query, key_cache, value_cache, alibi_slopes, block_seq, block_pos, lengths, out_weight.T)

    placed = (
        P(("group", "seq"), "tensor"),
        P(("group", "seq"), None, "tensor"),
        P(("group", "seq"), None, "tensor"),
        P("tensor"),
        P(("group", "seq")),
        P(("group", "seq")),
        P("group"),
        P("tensor", "seq"),
    )
    return jax.shard_map(
        local, mesh=mesh, in_specs=placed, out_specs=P(("group", "tensor"), "seq"), check_vma=False
    )
```

```python
import functools
import math

import jax
import jax.numpy as jnp
from jax import lax
from jax.experimental import pallas as pl
from jax.experimental.pallas import tpu as pltpu
from jax.sharding import PartitionSpec as P

MESH = pl.DeviceIdType.MESH
F32 = jnp.float32
BF16 = jnp.bfloat16
CORES = 2
LATE = 3
GONE = -1e30


def remote(src, dst, send, recv, where):
    return pltpu.make_async_remote_copy(
        src_ref=src, dst_ref=dst, send_sem=send, recv_sem=recv, device_id=where, device_id_type=MESH
    )


def spread(slots, chips, z, c, send, recv, relay):
    partner = {"seq": z * CORES + 1 - c}
    for chip in range(chips):

        @pl.when(chip != z)
        def _():
            behind = lax.rem(chip - z + chips, chips)
            there = {"seq": chip * CORES + c}
            remote(slots.at[c, 0], slots.at[c, behind], send, recv.at[0], there).start()

    every = pl.ds(0, chips - 1)
    remote(slots.at[c, every], slots.at[c, every], send, recv.at[0], partner).wait_recv()
    half = remote(slots.at[c], slots.at[c], relay.at[0], relay.at[1], partner)
    half.start()
    half.wait_recv()

    def drain():
        half.wait_send()
        remote(slots.at[c, every], slots.at[c, every], send, relay.at[1], partner).wait_send()

    return drain


def far_first(n):
    return sorted(range(1, n), key=lambda m: -min(m, n - m))


def kernel(
    chips, owners, heads,
    q_hbm, k_hbm, v_hbm, slopes_hbm, block_seq_hbm, block_pos_hbm, lengths_hbm, w_hbm, out,
    slopes, block_seq, block_pos, lengths, kbuf, kturn, vbuf, wbuf, qall, gall, part, landed,
    load, met, ready, e_send, f_send, f_recv, e_recv, r_recv, d_recv, q_send, q_recv, g_send, g_recv, g_relay, p_send, p_recv,
):
    seq = lax.axis_index("seq")
    mine = lax.axis_index("tensor")
    devices = CORES * chips
    z, c = seq // CORES, lax.rem(seq, CORES)
    blocks, block_len, features = k_hbm.shape
    rows = q_hbm.shape[0]
    head_dim = features // heads
    seqs = lengths_hbm.shape[0]
    scale = 1.0 / math.sqrt(head_dim)

    order = sorted(range(owners), key=lambda x: (min(x, owners - x), x * 2 <= owners))
    order = order[:-3] + [owners // 2] + [x for x in order[-3:] if x * 2 != owners]
    rank = sum(jnp.where(mine == x, r, 0) for r, x in enumerate(order))

    first_late = chips - LATE

    barrier = pltpu.get_barrier_semaphore()

    def greet_seq(j, _):
        pl.semaphore_signal(barrier, inc=1, device_id={"seq": j}, device_id_type=MESH)
        return 0

    q_load = pltpu.make_async_copy(q_hbm, qall.at[seq], load.at[0])
    q_load.start()

    @pl.when(seq > 0)
    def _():
        lax.fori_loop(seq + 1, devices, greet_seq, 0)

    @pl.when(seq == 1)
    def _():
        greet_seq(0, 0)

    for r, x in enumerate(order):

        @pl.when((r > rank) & (seq == 1))
        def _(x=x):
            pl.semaphore_signal(barrier, inc=1, device_id={"tensor": x}, device_id_type=MESH)


    small = [
        pltpu.make_async_copy(src, dst, load.at[4 + i])
        for i, (src, dst) in enumerate(
            (
                (slopes_hbm, slopes),
                (block_seq_hbm, block_seq),
                (block_pos_hbm, block_pos),
                (lengths_hbm, lengths),
            )
        )
    ]
    k_load = pltpu.make_async_copy(k_hbm, kbuf, load.at[1])
    v_load = pltpu.make_async_copy(v_hbm, vbuf, load.at[2])
    w_load = pltpu.make_async_copy(w_hbm, wbuf, load.at[3])
    for copy in small:
        copy.start()
    k_load.start()
    v_load.start()
    w_load.start()
    q_load.wait()
    before = jnp.where(seq == 0, 1, jnp.where(seq == 1, rank, seq - 1))

    @pl.when(before > 0)
    def _():
        pl.semaphore_wait(barrier, before)

    def give_q(j):
        return remote(qall.at[seq], qall.at[seq], q_send, q_recv.at[seq], {"seq": j})

    def arrival(j):
        return remote(qall.at[j], qall.at[j], q_send, q_recv.at[j], {"seq": z * CORES + 1 - c})

    def several(slots, recv, j, send=q_send):
        return remote(qall.at[slots], qall.at[slots], send, recv, {"seq": j})

    pair = pl.ds(0, CORES)
    rest = pl.ds(1, devices - 1)

    def early(core):
        return pl.ds(core * first_late, first_late)

    def send_down(i, _):
        far = chips // 2
        step = (i + 1) // 2
        k = jnp.where(lax.rem(i, 2) == 0, far - step, far + step)
        for cc in range(CORES):
            j = lax.rem(z + k, chips) * CORES + cc

            @pl.when((j > 0) & (j < seq))
            def _():
                give_q(j).start()

        return 0

    lax.fori_loop(0, chips, send_down, 0)

    for r, x in enumerate(order):

        @pl.when((r < rank) & (seq == 1))
        def _(x=x):
            pl.semaphore_signal(met, inc=1, device_id={"tensor": x}, device_id_type=MESH)

    k_load.wait()
    for b in range(blocks):
        kturn[b] = kbuf[b].T

    def arrive(j, _):
        arrival(j).wait_recv()
        return 0

    @pl.when(seq == 0)
    def _():
        give_q(1).start()
        several(rest, r_recv, 1).wait_recv()

    @pl.when(seq == 1)
    def _():
        arrival(0).wait_recv()

        def pass_pair(j, _):
            arrival(j).wait_recv()
            several(pair, f_recv, j, f_send).start()
            return 0

        lax.fori_loop(CORES, first_late * CORES, pass_pair, 0)

        def pass_early(j, _):
            arrival(j).wait_recv()
            several(early(lax.rem(j, CORES)), e_recv, j, e_send.at[j - first_late * CORES]).start()
            return 0

        lax.fori_loop(first_late * CORES, devices, pass_early, 0)
        several(rest, r_recv, 0).start()

        @pl.when(rank < owners - 1)
        def _():
            pl.semaphore_wait(met, owners - 1 - rank)

        for step in range(1, owners):
            there = {"tensor": lax.rem(mine + step, owners)}
            pl.semaphore_signal(ready, inc=1, device_id=there, device_id_type=MESH)


    @pl.when(seq > 1)
    def _():
        def send_up(j, _):
            arrival(j).wait_recv()

            @pl.when((j < first_late * CORES) | (z >= first_late))
            def _():
                give_q(j).start()

            return 0

        lax.fori_loop(seq + 1, devices, send_up, 0)

        @pl.when(z >= first_late)
        def _():
            several(early(c), e_recv, 1).wait_recv()
            several(early(c), d_recv, z * CORES + 1 - c, f_send).start()
            lax.fori_loop(first_late * CORES, seq, arrive, 0)
            several(early(1 - c), d_recv, 1).wait_recv()

        @pl.when(z < first_late)
        def _():
            several(pair, f_recv, 1).wait_recv()
            lax.fori_loop(CORES, seq, arrive, 0)

    def q_drain():
        @pl.when(seq == 0)
        def _():
            give_q(1).wait_send()

        @pl.when(seq == 1)
        def _():
            several(rest, r_recv, 0).wait_send()
            size = kbuf.at[0, pl.ds(0, (first_late - 1) * CORES * CORES * rows)]
            remote(size, size, f_send, r_recv, {"seq": 0}).wait_send()
            for i in range(LATE * CORES):
                several(early(0), e_recv, 0, e_send.at[i]).wait_send()

        @pl.when((seq > 1) & (z < first_late))
        def _():
            several(pl.ds(0, devices - 2 - LATE * CORES), r_recv, 1).wait_send()

        @pl.when(z >= first_late)
        def _():
            several(pl.ds(0, devices - 2), r_recv, 1).wait_send()
            several(early(c), r_recv, 1, f_send).wait_send()

    sub = lax.broadcasted_iota(jnp.int32, (8, features), 0)
    lane = lax.broadcasted_iota(jnp.int32, (8, features), 1)
    own_head = lane // head_dim == sub
    t_at = lax.broadcasted_iota(jnp.int32, (8, block_len), 1)
    h_at = lax.broadcasted_iota(jnp.int32, (8, block_len), 0)
    a_sub = lax.broadcasted_iota(jnp.int32, (8, head_dim), 0)
    a_lane = lax.broadcasted_iota(jnp.int32, (8, head_dim), 1)

    v_load.wait()
    for copy in small:
        copy.wait()
    slope = jnp.zeros((8, block_len), F32)
    for h in range(heads):
        slope = jnp.where(h_at == h, slopes[h], slope)
    wholes = []
    for b in range(blocks):
        s = block_seq[b]
        length = lengths[s]
        owner = s // rows
        r = lax.rem(s, rows)
        pair = qall[owner].astype(F32)
        row = pair[0:1]
        for i in range(1, rows):
            row = jnp.where(r == i, pair[i : i + 1], row)
        wide = jnp.where(own_head, jnp.broadcast_to(row, (8, features)), 0.0).astype(BF16)
        scores = lax.dot_general(
            wide, kturn[b], (((1,), (0,)), ((), ())), preferred_element_type=F32
        )
        placed = block_pos[b] * block_len + t_at
        live = placed < length
        distance = (length - 1 - placed).astype(F32)
        scores = jnp.where(live, scores * scale - slope * distance, GONE)
        top = jnp.max(scores, axis=1, keepdims=True)
        weights = jnp.where(live, jnp.exp(scores - top), 0.0)
        total = jnp.sum(weights, axis=1, keepdims=True)
        acc = jnp.dot(weights.astype(BF16), vbuf[b], preferred_element_type=F32)
        o = jnp.sum(jnp.where(own_head, acc * (1.0 / total), 0.0), axis=0, keepdims=True)
        lse = top + jnp.log(total)
        high = lse.astype(BF16).astype(F32)
        mid = (lse - high).astype(BF16).astype(F32)
        low = lse - high - mid
        tail = jnp.where(a_lane == a_sub, high, 0.0)
        tail = jnp.where(a_lane == a_sub + 8, mid, tail)
        tail = jnp.where(a_lane == a_sub + 16, low, tail)
        tail = jnp.where((a_lane == 24) & (a_sub == 0), s.astype(F32), tail)
        tail = jnp.sum(jnp.where(a_sub < heads, tail, 0.0), axis=0, keepdims=True)
        wholes.append(jnp.concatenate([o, tail], axis=1))

    wide = 2 * head_dim
    groups = (heads + 1) // 2
    m_sub = lax.broadcasted_iota(jnp.int32, (8, wide), 0)
    halves = []
    for first in range(0, groups * blocks, 8):
        half = jnp.zeros((8, wide), F32)
        for i in range(8):
            j, b = divmod(first + i, blocks)
            piece = wholes[b][:, j * wide : (j + 1) * wide]
            half = jnp.where(m_sub == i, jnp.broadcast_to(piece, (8, wide)), half)
        halves.append(half)
    gall[c, 0] = jnp.concatenate(halves, axis=0).astype(BF16)

    @pl.when(seq == 1)
    def _():
        pl.semaphore_wait(ready, owners - 1)

    g_drain = spread(gall, chips, z, c, g_send, g_recv, g_relay)

    high_rows = groups * blocks
    count = CORES * chips * high_rows
    both = gall[...].reshape(count, wide)
    p_sub = lax.broadcasted_iota(jnp.int32, (16, head_dim), 0)
    p_lane = lax.broadcasted_iota(jnp.int32, (16, head_dim), 1)
    pick = (p_sub < 8) & (p_lane < 24) & (lax.rem(p_lane, 8) == p_sub)
    pick = pick | ((p_sub == 8) & (p_lane == 24))
    pick = jnp.where(pick, 1.0, 0.0).astype(BF16)
    tails = lax.dot_general(
        pick, both[:, head_dim:], (((1,), (1,)), ((), ())), preferred_element_type=F32
    )
    column = lax.broadcasted_iota(jnp.int32, (seqs, count), 1)
    group_of = lax.rem(column // blocks, groups)
    seq_at = lax.broadcasted_iota(jnp.int32, (seqs, count), 0).astype(F32)
    shares, inverse = [], []
    for j in range(groups):
        back = (groups - 1 - j) * blocks
        moved = tails if back == 0 else pltpu.roll(tails, count - back, 1)
        mask = (group_of == j) & (jnp.broadcast_to(moved[8:9], (seqs, count)) == seq_at)
        for h in range(2 * j, min(2 * j + 2, heads)):
            level = jnp.where(mask, jnp.broadcast_to(moved[h : h + 1], (seqs, count)), GONE)
            best = jnp.max(level, axis=1, keepdims=True)
            share = jnp.exp(level - best)
            inverse.append(1.0 / jnp.sum(share, axis=1, keepdims=True))
            shares.append(share.astype(BF16))
    mixed = jnp.dot(jnp.concatenate(shares, axis=0), both, preferred_element_type=F32)
    attention = jnp.concatenate(
        [
            (
                mixed[h * seqs : (h + 1) * seqs, (h % 2) * head_dim : (h % 2 + 1) * head_dim] * inverse[h]
            ).astype(BF16)
            for h in range(heads)
        ],
        axis=1,
    )
    w_load.wait()
    product = lax.dot_general(
        attention, wbuf[...], (((1,), (1,)), ((), ())), preferred_element_type=F32
    )
    share_rows = seqs // owners
    for x in range(owners):
        part[x] = product[x * share_rows : (x + 1) * share_rows].astype(BF16)

    def give(k):
        there = lax.rem(mine + k, owners)
        return remote(part.at[there], landed.at[k - 1], p_send, p_recv, {"tensor": there})

    for k in far_first(owners):
        give(k).start()
    result = part[mine].astype(F32)

    others = pl.ds(0, owners - 1)
    all_others = remote(part.at[others], landed.at[others], p_send, p_recv, {"tensor": mine})
    all_others.wait_recv()
    for k in range(1, owners):
        result = result + landed[k - 1].astype(F32)
    out[...] = result.astype(BF16)

    q_drain()
    g_drain()

    all_others.wait_send()


def solution(mesh):
    chips = mesh.shape["seq"] // CORES
    owners = mesh.shape["tensor"]

    def local(query, key_cache, value_cache, alibi_slopes, block_seq, block_pos, lengths, out_weight):
        heads = alibi_slopes.shape[0]
        rows, features = query.shape
        blocks, block_len, _ = key_cache.shape
        seqs = lengths.shape[0]
        columns = out_weight.shape[1]
        head_dim = features // heads
        message = ((heads + 1) // 2 * blocks, 2 * head_dim)
        hbm = pl.BlockSpec(memory_space=pltpu.HBM)
        dma = pltpu.SemaphoreType.DMA
        return pl.pallas_call(
            functools.partial(kernel, chips, owners, heads),
            out_shape=pltpu.VMEM((seqs // owners, columns), BF16),
            in_specs=[hbm] * 8,
            out_specs=pl.BlockSpec(memory_space=pltpu.VMEM),
            scratch_shapes=[
                pltpu.SMEM(alibi_slopes.shape, F32),
                pltpu.SMEM(block_seq.shape, jnp.int32),
                pltpu.SMEM(block_pos.shape, jnp.int32),
                pltpu.SMEM(lengths.shape, jnp.int32),
                pltpu.VMEM(key_cache.shape, BF16),
                pltpu.VMEM((blocks, features, block_len), BF16),
                pltpu.VMEM(value_cache.shape, BF16),
                pltpu.VMEM(out_weight.shape[::-1], BF16),
                pltpu.VMEM((CORES * chips, rows, features), BF16),
                pltpu.VMEM((CORES, chips, *message), BF16),
                pltpu.VMEM((owners, seqs // owners, columns), BF16),
                pltpu.VMEM((owners, seqs // owners, columns), BF16),
                dma((8,)),
                pltpu.SemaphoreType.REGULAR,
                pltpu.SemaphoreType.REGULAR,
                dma((LATE * CORES,)),
                dma,
                dma,
                dma,
                dma,
                dma,
                dma,
                dma((CORES * chips,)),
                dma,
                dma((1,)),
                dma((2,)),
                dma,
                dma,
            ],
            compiler_params=pltpu.CompilerParams(
                collective_id=0, has_side_effects=True
            ),
        )(query, key_cache, value_cache, alibi_slopes, block_seq, block_pos, lengths, out_weight.T)

    placed = (
        P(("group", "seq"), "tensor"),
        P(("group", "seq"), None, "tensor"),
        P(("group", "seq"), None, "tensor"),
        P("tensor"),
        P(("group", "seq")),
        P(("group", "seq")),
        P("group"),
        P("tensor", "seq"),
    )
    return jax.shard_map(
        local, mesh=mesh, in_specs=placed, out_specs=P(("group", "tensor"), "seq"), check_vma=False
    )
```
